256 devices in a mesh: krow: 32 (over x, z_lo, y), col: 8 (over z_hi, core).
Axes of the slice: x: 4, y: 4, z: 8 (z_hi: 4, z_lo: 2; z = z_hi * 2 + z_lo), core: 2. Of those that a mesh axis runs over, the one named last changes fastest.
Arguments:
- features: bfloat16 [16384, 6144], P('krow', 'col'), may hold values from -9 to 9
- slab: bfloat16 [16384, 2048], P('krow', 'col'), may hold values from -9 to 9
- pack_order: int32 [32, 512], P('krow'), may hold values from 0 to 511, each once within a row
- place_order: int32 [32, 512], P('krow'), may hold values from 0 to 511, each once within a row
- start: int32 [1], replicated, may hold values from 512 to 2048
Outputs:
- factored: float32 [16384, 1024], P(('krow', 'col'))
The draws below stay inside these ranges and needn't reach their ends.
Inputs may be any that keep to these rules, and one draw needn't show every extreme that they name: Row k of krow device s's sending order is its local row pack_order[s, k]. `place_order`: each krow device's elimination rows are a rearrangement of the rows it receives. Slab columns from start[0] on are not yet computed and are ignored.
All inputs are finite; a program needn't handle non-finite values.
Results may differ from the reference program's by a relative error of at most 0.0003.
Values may be sent and summed in bfloat16 or wider, within the bound.
No kernel may reach another device: no remote copies, remote signals or barrier semaphores. Data moves between devices by JAX's collectives and lax.ppermute only.
A program may use at most 64 MiB of HBM per device.

```python
import jax
import jax.numpy as jnp
from jax import lax

F = 6144
PW = 512
R_DEV = 512
ROWS = 16384
PRIOR = 2048
N_KROW = 32


def draw_features(key, part):
    first = jax.random.fold_in(key, 11)
    second = jax.random.fold_in(key, 12)
    third = jax.random.fold_in(key, 13)
    latent = jax.random.normal(first, (ROWS, 8), jnp.float32) * 8.0 ** (-0.5)
    basis = jax.random.normal(second, (8, F), jnp.float32)
    noise = 0.5 * jax.random.normal(third, (ROWS, F), jnp.float32)
    values = jnp.dot(latent, basis, precision=lax.Precision.HIGHEST) + noise
    return jnp.clip(values, -9.0, 9.0).astype(jnp.bfloat16)


def draw_slab(key, part):
    first = jax.random.fold_in(key, 21)
    base = jnp.clip(jax.random.normal(first, (ROWS, PRIOR), jnp.float32), -6.0, 6.0)
    rowscale = jnp.ones((ROWS, 1), jnp.float32)
    upper = (jnp.arange(ROWS) < 2 * PW)[:, None]
    scale = jnp.where(upper, 0.002, 1.5 * rowscale)
    return jnp.clip(base * scale, -9.0, 9.0).astype(jnp.bfloat16)


def setup_inputs(seed: int = 0) -> dict:
    streams_of = jax.random.split(jax.random.key(seed), 6)
    features = draw_features(jax.random.fold_in(streams_of[5], 71), 0)
    slab = draw_slab(jax.random.fold_in(streams_of[5], 71), 0)
    pack_order = jax.vmap(lambda own: jax.random.permutation(own, R_DEV))(jax.random.split(streams_of[2], N_KROW)).reshape((N_KROW, R_DEV)).astype(jnp.int32)
    place_order = jax.vmap(lambda own: jax.random.permutation(own, R_DEV))(jax.random.split(streams_of[3], N_KROW)).reshape((N_KROW, R_DEV)).astype(jnp.int32)
    start = jax.random.randint(streams_of[4], (1,), PRIOR // 4, PRIOR + 1).astype(jnp.int32)
    return dict(features=features, slab=slab, pack_order=pack_order, place_order=place_order, start=start)


RIDGE = 0.5

def reference(features, slab, pack_order, place_order, start):
    group = R_DEV // N_KROW
    senders = (jnp.arange(N_KROW)[:, None] * R_DEV + pack_order).reshape(-1).astype(jnp.int32)
    packed = jnp.take(features, senders, axis=0)
    blocks = packed.reshape(N_KROW, N_KROW, group, F)
    arrived = jnp.transpose(blocks, (1, 0, 2, 3)).reshape(ROWS, F)
    placing = (jnp.arange(N_KROW)[:, None] * R_DEV + place_order).reshape(-1).astype(jnp.int32)
    ordered = jnp.take(arrived, placing, axis=0)
    norms = jnp.sum(jnp.square(ordered.astype(jnp.float32)), axis=1)
    kept = (jnp.arange(PRIOR) < start[0])[None, :]
    keep = jnp.where(kept, slab, jnp.zeros((), jnp.bfloat16))
    positions = jnp.arange(ROWS)
    outputs = []
    earlier = None
    for panel in range(2):
        lower = panel * PW
        targets = lower + jnp.arange(PW)
        gram = jnp.dot(ordered.astype(jnp.float32), ordered[lower:lower + PW].T.astype(jnp.float32), preferred_element_type=jnp.float32)
        dist = norms[:, None] + norms[lower:lower + PW][None, :] - 2.0 * gram
        update = jnp.dot(keep.astype(jnp.float32), keep[lower:lower + PW].T.astype(jnp.float32), preferred_element_type=jnp.float32)
        shift = (positions[:, None] == targets[None, :]).astype(jnp.float32)
        matrix = jnp.exp(-dist / (2.0 * F)) + RIDGE * shift - update
        if earlier is not None:
            matrix = matrix - jnp.dot(earlier, earlier[lower:lower + PW].T, precision=lax.Precision.HIGHEST)
        factor = jnp.linalg.cholesky(matrix[lower:lower + PW])
        solved = jax.scipy.linalg.solve_triangular(factor, matrix.T, lower=True).T
        solved = jnp.where((positions >= lower)[:, None], solved, jnp.zeros((), jnp.float32))
        outputs.append(solved)
        earlier = solved
    return jnp.concatenate(outputs, axis=1)
```

```python
import jax
import jax.numpy as jnp
from jax import lax
from jax.sharding import PartitionSpec as P

F = 6144
PW = 512
TOP = 2 * PW
BK = 128
RIDGE = 0.5


def swap(value, axis):
    return lax.all_to_all(value, axis, split_axis=0, concat_axis=0, tiled=True)


def from_everyone(value, axis):
    return swap(jnp.broadcast_to(value, (lax.axis_size(axis), *value.shape)), axis)


def sq_norms(rows):
    return jnp.sum(jnp.square(rows.astype(jnp.float32)), axis=1)


def inner(a, b):
    return lax.dot_general(a, b, (((1,), (1,)), ((), ())), preferred_element_type=jnp.float32)


def fold(upper, lower, pair):
    blocks = []
    for slot in range(9):
        hi = upper[:, slot * BK:(slot + 1) * BK] if slot < 8 else None
        at = 8 - slot
        lo = lower[:, at * BK:(at + 1) * BK] if slot > 4 else None
        if lo is None:
            blocks.append(hi)
        elif hi is None:
            blocks.append(lo)
        else:
            blocks.append(jnp.where(slot + pair <= 7, hi, lo))
    return jnp.concatenate(blocks, axis=1)


def unfold(folded):
    rows = []
    for r in range(8):
        if r >= 4:
            b = 7 - r
            part = folded[b * BK:(b + 1) * BK, :(r + 1) * BK]
        else:
            part = jnp.concatenate(
                [folded[r * BK:(r + 1) * BK, (8 - j) * BK:(9 - j) * BK] for j in range(r + 1)], axis=1)
        rows.append(jnp.pad(part, ((0, 0), (0, TOP - part.shape[1]))))
    return jnp.concatenate(rows, axis=0)


def factor_and_solve(folded, matrix):
    top = unfold(folded)
    factor = lax.linalg.cholesky(top, symmetrize_input=False)
    return jax.scipy.linalg.solve_triangular(factor, matrix.T, lower=True).T


def shards(features, slab, pack_order, place_order, start):
    n_krow, n_col = lax.axis_size("krow"), lax.axis_size("col")
    rows_dev = features.shape[0]
    group = rows_dev // n_krow
    prior_dev = slab.shape[1]
    krow, col = lax.axis_index("krow"), lax.axis_index("col")

    kept = (col * prior_dev + jnp.arange(prior_dev) < start[0])[None, :]
    slab_part = swap(slab, "krow")[:2 * group]
    places = from_everyone(place_order, "krow")[:2, 0]
    packed = jnp.take(features, pack_order[0], axis=0)
    top_arrived = from_everyone(packed[:2 * group], "krow")
    top_slab = from_everyone(slab_part, "krow")
    arrived = swap(packed, "krow")

    def by_panel(tiles):
        width = tiles.shape[-1]
        tiles = tiles.reshape(n_krow, 2, group, width)
        return jnp.moveaxis(tiles, 1, 0).reshape(TOP, width)

    top_feats = by_panel(top_arrived)
    wanted = (places + jnp.arange(2)[:, None] * rows_dev).reshape(TOP)
    top_feats = jnp.take(top_feats, wanted, axis=0)
    top_slab = jnp.where(kept, by_panel(top_slab), jnp.zeros((), jnp.bfloat16))
    top_norms = sq_norms(top_feats)

    share = PW // n_krow
    at = krow * share
    pair = at // BK
    row_lo = at
    row_hi = (7 - pair) * BK + (at - pair * BK)

    def rows_of(array, first):
        return lax.dynamic_slice_in_dim(array, first, share, 0)

    def both(array):
        return jnp.concatenate([rows_of(array, row_hi), rows_of(array, row_lo)], axis=0)

    gram = inner(both(top_feats), top_feats)
    dist = both(top_norms)[:, None] + top_norms[None, :] - 2.0 * gram
    update = inner(both(top_slab), top_slab)
    dist = fold(dist[:share], dist[share:], pair)
    update = fold(update[:share], update[share:], pair)
    parts = jnp.concatenate([dist, update], axis=1)
    summed = jnp.sum(swap(parts, "col").reshape(n_col, share // n_col, 2 * 9 * BK), axis=0)
    dist, update = summed[:, :9 * BK], summed[:, 9 * BK:]
    mine = share // n_col
    col_ids = jnp.arange(TOP)[None, :]
    ids = jnp.arange(mine)[:, None] + col * mine
    shift = fold((row_hi + ids == col_ids).astype(jnp.float32),
                 (row_lo + ids == col_ids).astype(jnp.float32), pair)
    entries = jnp.exp(-dist / (2.0 * F)) + RIDGE * shift - update
    entries = from_everyone(entries, "col").reshape(share, 9 * BK)
    folded = from_everyone(entries, "krow").reshape(PW, 9 * BK)

    ordered = jnp.take(arrived, place_order[0], axis=0)
    dist = sq_norms(ordered)[:, None] + top_norms[None, :] - 2.0 * inner(ordered, top_feats)
    update = inner(slab, top_slab)
    parts = lax.psum_scatter(jnp.concatenate([dist, update], axis=1), "col", scatter_dimension=0, tiled=True)
    dist, update = parts[:, :TOP], parts[:, TOP:]
    own = rows_dev // n_col
    positions = krow * rows_dev + col * own + jnp.arange(own)
    shift = (positions[:, None] == col_ids).astype(jnp.float32)
    matrix = jnp.exp(-dist / (2.0 * F)) + RIDGE * shift - update

    solved = factor_and_solve(folded, matrix)
    return jnp.where((positions[:, None] >= PW) | (col_ids < PW), solved, 0.0)


def solution(mesh):
    in_specs = (P("krow", "col"), P("krow", "col"), P("krow", None), P("krow", None), P())
    out_specs = P(("krow", "col"), None)
    return jax.shard_map(shards, mesh=mesh, in_specs=in_specs, out_specs=out_specs, check_vma=False)
```

```python
import jax
import jax.numpy as jnp
from jax import lax
from jax.experimental import pallas as pl
from jax.experimental.pallas import tpu as pltpu
from jax.sharding import PartitionSpec as P

F = 6144
PW = 512
TOP = 2 * PW
BK = 128
OWN = 64
CODE = 32
RIDGE = 0.5
HI = lax.Precision.HIGHEST

def swap(value, axis):
    return lax.all_to_all(value, axis, split_axis=0, concat_axis=0, tiled=True)


def from_everyone(value, axis):
    return swap(jnp.broadcast_to(value, (lax.axis_size(axis), *value.shape)), axis)


def sq_norms(rows):
    return jnp.sum(jnp.square(rows.astype(jnp.float32)), axis=1)


def inner(a, b):
    return lax.dot_general(a, b, (((1,), (1,)), ((), ())), preferred_element_type=jnp.float32)


def fold(upper, lower, pair):
    blocks = []
    for slot in range(9):
        hi = upper[:, slot * BK:(slot + 1) * BK] if slot < 8 else None
        at = 8 - slot
        lo = lower[:, at * BK:(at + 1) * BK] if slot > 4 else None
        if lo is None:
            blocks.append(hi)
        elif hi is None:
            blocks.append(lo)
        else:
            blocks.append(jnp.where(slot + pair <= 7, hi, lo))
    return jnp.concatenate(blocks, axis=1)


def dot_t(a, b):
    return lax.dot_general(a, b, (((1,), (1,)), ((), ())), precision=HI, preferred_element_type=jnp.float32)

def over_rows(v, k):
    return jnp.broadcast_to(v[k:k + 1, :], v.shape)

def over_lanes(v, c):
    return jnp.broadcast_to(v[:, c:c + 1], v.shape)

def invert_factor(tiles, w_ref):
    n = len(tiles)
    lane = lax.broadcasted_iota(jnp.int32, (8, BK), 1)
    sub = lax.broadcasted_iota(jnp.int32, (8, BK), 0)
    for g in range(n):
        c0 = 8 * g
        top = tiles[g]
        cols = [over_lanes(top, c0 + k) for k in range(8)]
        cross, inv, rows = {}, [], []
        pivots = jnp.ones((8, BK), jnp.float32)
        for k in range(8):
            p = over_rows(cols[k], k)
            r = 1.0 / p
            row = jnp.where(lane == c0 + k, p + 1.0, over_rows(top, k))
            m = jnp.where(sub > k, cols[k] * r, 0.0)
            for k2 in range(k + 1, 8):
                cross[k, k2] = over_rows(cols[k2], k)
                cols[k2] = cols[k2] - m * cross[k, k2]
            top = top - m * row
            pivots = jnp.where(sub == k, p, pivots)
            inv.append(r)
            rows.append(row)
        unit = jnp.where(lane < c0 + sub, top, jnp.where(lane == c0 + sub, 1.0, 0.0))
        w_ref[c0:c0 + 8, :] = unit * lax.rsqrt(pivots)
        for i in range(g + 1, n):
            tile = tiles[i]
            cols = [over_lanes(tile, c0 + k) for k in range(8)]
            for k in range(8):
                m = cols[k] * inv[k]
                for k2 in range(k + 1, 8):
                    cols[k2] = cols[k2] - m * cross[k, k2]
                tile = tile - m * rows[k]
            tiles[i] = tile

def chol_kernel(f_ref, m_ref, o_ref, a_ref, w_ref):
    nb = TOP // BK
    for r in range(nb):
        if r >= nb // 2:
            b = nb - 1 - r
            a_ref[r * BK:(r + 1) * BK, :(r + 1) * BK] = f_ref[b * BK:(b + 1) * BK, :(r + 1) * BK]
        else:
            for j in range(r + 1):
                a_ref[r * BK:(r + 1) * BK, j * BK:(j + 1) * BK] = f_ref[r * BK:(r + 1) * BK, (nb - j) * BK:(nb + 1 - j) * BK]
    a_ref[TOP:, :] = m_ref[...]

    def step(j, carry):
        o = pl.multiple_of(j * BK, BK)
        tiles = [a_ref[pl.ds(pl.multiple_of(o + 8 * i, 8), 8), pl.ds(o, BK)] for i in range(BK // 8)]
        invert_factor(tiles, w_ref)
        for b in range(nb):
            @pl.when(j == b)
            def _():
                lo, hi = b * BK, (b + 1) * BK
                panel = dot_t(a_ref[hi:, lo:hi], w_ref[...])
                o_ref[:, lo:hi] = panel[TOP - hi:, :]
                for c in range(b + 1, nb):
                    at = c * BK
                    a_ref[at:, at:at + BK] -= dot_t(panel[at - hi:, :], panel[at - hi:at - hi + BK, :])
        return carry
    lax.fori_loop(0, nb, step, 0)

def factor_and_solve(folded, matrix):
    return pl.pallas_call(
        chol_kernel,
        out_shape=jax.ShapeDtypeStruct(matrix.shape, jnp.float32),
        in_specs=[pl.BlockSpec(memory_space=pltpu.VMEM)] * 2,
        out_specs=pl.BlockSpec(memory_space=pltpu.VMEM),
        scratch_shapes=[pltpu.VMEM((TOP + OWN, TOP), jnp.float32), pltpu.VMEM((BK, BK), jnp.float32)],
    )(folded, matrix)


def shards(features, slab, pack_order, place_order, start):
    n_krow, n_col = lax.axis_size("krow"), lax.axis_size("col")
    rows_dev = features.shape[0]
    group = rows_dev // n_krow
    prior_dev = slab.shape[1]
    krow, col = lax.axis_index("krow"), lax.axis_index("col")

    kept = (col * prior_dev + jnp.arange(prior_dev) < start[0])[None, :]
    order = place_order[0]
    coded = jnp.stack([order // CODE, order % CODE], axis=1).astype(jnp.bfloat16)
    coded = jnp.pad(coded, ((0, 0), (0, BK - 2)))
    slab_part = swap(jnp.concatenate([slab, coded], axis=1), "krow")[:2 * group]
    packed = jnp.take(features, pack_order[0], axis=0)
    feat_dev = packed.shape[1]
    tiles = from_everyone(jnp.concatenate([packed[:2 * group], slab_part], axis=1), "krow")
    packed, tiles = lax.optimization_barrier((packed, tiles))
    arrived = swap(packed, "krow")

    tiles = tiles.reshape(n_krow, 2, group, tiles.shape[-1])
    top = jnp.moveaxis(tiles, 1, 0).reshape(TOP, tiles.shape[-1])
    places = top[:, feat_dev + prior_dev:feat_dev + prior_dev + 2].astype(jnp.float32).astype(jnp.int32)
    wanted = places[:, 0] * CODE + places[:, 1] + jnp.arange(TOP) // rows_dev * rows_dev
    top_feats = jnp.take(top[:, :feat_dev], wanted, axis=0)
    top_slab = jnp.where(kept, top[:, feat_dev:feat_dev + prior_dev], jnp.zeros((), jnp.bfloat16))
    top_norms = sq_norms(top_feats)

    share = PW // n_krow
    at = krow * share
    pair = at // BK
    row_lo = at
    row_hi = (7 - pair) * BK + (at - pair * BK)

    def rows_of(array, first):
        return lax.dynamic_slice_in_dim(array, first, share, 0)

    def both(array):
        return jnp.concatenate([rows_of(array, row_hi), rows_of(array, row_lo)], axis=0)

    gram = inner(both(top_feats), top_feats)
    dist = both(top_norms)[:, None] + top_norms[None, :] - 2.0 * gram
    update = inner(both(top_slab), top_slab)
    dist = fold(dist[:share], dist[share:], pair)
    update = fold(update[:share], update[share:], pair)
    parts = jnp.concatenate([dist, update], axis=1)
    parts, arrived = lax.optimization_barrier((parts, arrived))
    summed = jnp.sum(swap(parts, "col").reshape(n_col, share // n_col, 2 * 9 * BK), axis=0)
    dist, update = summed[:, :9 * BK], summed[:, 9 * BK:]
    mine = share // n_col
    col_ids = jnp.arange(TOP)[None, :]
    ids = jnp.arange(mine)[:, None] + col * mine
    shift = fold((row_hi + ids == col_ids).astype(jnp.float32),
                 (row_lo + ids == col_ids).astype(jnp.float32), pair)
    entries = jnp.exp(-dist / (2.0 * F)) + RIDGE * shift - update
    entries = from_everyone(entries, "col").reshape(share, 9 * BK)
    folded = from_everyone(entries, "krow").reshape(PW, 9 * BK)

    ordered = jnp.take(arrived, place_order[0], axis=0)
    dist = sq_norms(ordered)[:, None] + top_norms[None, :] - 2.0 * inner(ordered, top_feats)
    update = inner(slab, top_slab)
    parts = lax.psum_scatter(jnp.concatenate([dist, update], axis=1), "col", scatter_dimension=0, tiled=True)
    dist, update = parts[:, :TOP], parts[:, TOP:]
    own = rows_dev // n_col
    positions = krow * rows_dev + col * own + jnp.arange(own)
    shift = (positions[:, None] == col_ids).astype(jnp.float32)
    matrix = jnp.exp(-dist / (2.0 * F)) + RIDGE * shift - update

    solved = factor_and_solve(folded, matrix)
    return jnp.where((positions[:, None] >= PW) | (col_ids < PW), solved, 0.0)


def solution(mesh):
    in_specs = (P("krow", "col"), P("krow", "col"), P("krow", None), P("krow", None), P())
    out_specs = P(("krow", "col"), None)
    return jax.shard_map(shards, mesh=mesh, in_specs=in_specs, out_specs=out_specs, check_vma=False)
```

```python
import jax
import jax.numpy as jnp
from jax import lax
from jax.experimental import pallas as pl
from jax.experimental.pallas import tpu as pltpu
from jax.sharding import PartitionSpec as P

F = 6144
PW = 512
TOP = 2 * PW
BK = 128
CODE = 32
RIDGE = 0.5
HI = lax.Precision.HIGHEST


def rows_at(array, where):
    return array.at[where].get(mode="promise_in_bounds", unique_indices=True)


def swap(value, axis):
    return lax.all_to_all(value, axis, split_axis=0, concat_axis=0, tiled=True)


def from_everyone(value, axis):
    return swap(jnp.broadcast_to(value, (lax.axis_size(axis), *value.shape)), axis)


def sq_norms(rows):
    return jnp.sum(jnp.square(rows.astype(jnp.float32)), axis=1)


def inner(a, b):
    return lax.dot_general(a, b, (((1,), (1,)), ((), ())), preferred_element_type=jnp.float32)


def fold(upper, lower, pair):
    blocks = []
    for slot in range(9):
        hi = upper[:, slot * BK:(slot + 1) * BK] if slot < 8 else None
        at = 8 - slot
        lo = lower[:, at * BK:(at + 1) * BK] if slot > 4 else None
        if lo is None:
            blocks.append(hi)
        elif hi is None:
            blocks.append(lo)
        else:
            blocks.append(jnp.where(slot + pair <= 7, hi, lo))
    return jnp.concatenate(blocks, axis=1)


def dot_t(a, b):
    return lax.dot_general(a, b, (((1,), (1,)), ((), ())), precision=HI, preferred_element_type=jnp.float32)


def over_rows(v, k):
    return jnp.broadcast_to(v[k:k + 1, :], v.shape)


def over_lanes(v, c):
    return jnp.broadcast_to(v[:, c:c + 1], v.shape)


def invert_factor(tiles, w_ref, first):
    n = len(tiles)
    lane = lax.broadcasted_iota(jnp.int32, (8, BK), 1)
    sub = lax.broadcasted_iota(jnp.int32, (8, BK), 0)
    for g in range(n):
        c0 = 8 * g
        top = tiles[g]
        cols = [over_lanes(top, c0 + k) for k in range(8)]
        cross, inv, rows = {}, [], []
        pivots = jnp.ones((8, BK), jnp.float32)
        for k in range(8):
            p = over_rows(cols[k], k)
            r = 1.0 / p
            row = jnp.where(lane == c0 + k, p + 1.0, over_rows(top, k))
            m = jnp.where(sub > k, cols[k] * r, 0.0)
            for k2 in range(k + 1, 8):
                cross[k, k2] = over_rows(cols[k2], k)
                cols[k2] = cols[k2] - m * cross[k, k2]
            top = top - m * row
            pivots = jnp.where(sub == k, p, pivots)
            inv.append(r)
            rows.append(row)
        unit = jnp.where(lane < c0 + sub, top, jnp.where(lane == c0 + sub, 1.0, 0.0))
        w_ref[pl.ds(pl.multiple_of(first + c0, 8), 8), :] = unit * lax.rsqrt(pivots)
        for i in range(g + 1, n):
            tile = tiles[i]
            cols = [over_lanes(tile, c0 + k) for k in range(8)]
            for k in range(8):
                m = cols[k] * inv[k]
                for k2 in range(k + 1, 8):
                    cols[k2] = cols[k2] - m * cross[k, k2]
                tile = tile - m * rows[k]
            tiles[i] = tile


def factor_kernel(core_ref, mine_ref, other_ref, a_ref, w_ref):
    nb = TOP // BK
    pieces = mine_ref.shape[0]
    half = mine_ref.shape[1]
    per = pieces // (nb // 2)

    def place(first, second):
        for b in range(nb // 2):
            for i in range(per):
                for h, ref in enumerate((first, second)):
                    src = ref[b * per + i]
                    at = i * 2 * half + h * half
                    r = nb - 1 - b
                    a_ref[r * BK + at:r * BK + at + half, :(r + 1) * BK] = src[:, :(r + 1) * BK]
                    for j in range(b + 1):
                        a_ref[b * BK + at:b * BK + at + half, j * BK:(j + 1) * BK] = (
                            src[:, (nb - j) * BK:(nb + 1 - j) * BK])

    @pl.when(core_ref[0] == 0)
    def _():
        place(mine_ref, other_ref)

    @pl.when(core_ref[0] != 0)
    def _():
        place(other_ref, mine_ref)

    def step(j, carry):
        o = pl.multiple_of(j * BK, BK)
        tiles = [a_ref[pl.ds(pl.multiple_of(o + 8 * i, 8), 8), pl.ds(o, BK)] for i in range(BK // 8)]
        invert_factor(tiles, w_ref, o)
        for b in range(nb - 1):
            @pl.when(j == b)
            def _():
                lo, hi = b * BK, (b + 1) * BK
                panel = dot_t(a_ref[hi:, lo:hi], w_ref[lo:hi, :])
                a_ref[hi:, lo:hi] = panel
                for c in range(b + 1, nb):
                    at = c * BK
                    a_ref[at:, at:at + BK] -= dot_t(panel[at - hi:, :], panel[at - hi:at - hi + BK, :])
        return carry

    lax.fori_loop(0, nb, step, 0)


def solve_kernel(first_ref, p0_ref, p1_ref, p2_ref, p3_ref, a_ref, w_ref, o_ref):
    nb = TOP // BK
    total = (p0_ref[...] + p1_ref[...]) + (p2_ref[...] + p3_ref[...])
    rows = total.shape[0]
    pos = first_ref[0] + lax.broadcasted_iota(jnp.int32, (rows, TOP), 0)
    col = lax.broadcasted_iota(jnp.int32, (rows, TOP), 1)
    shift = jnp.where(pos == col, RIDGE, 0.0)
    m = jnp.exp(total[:, :TOP] * (-1.0 / (2.0 * F))) + shift - total[:, TOP:]
    for b in range(nb):
        lo, hi = b * BK, (b + 1) * BK
        x = dot_t(m[:, :BK], w_ref[lo:hi, :])
        keep = (pos[:, lo:hi] >= PW) | (lo < PW)
        o_ref[:, lo:hi] = jnp.where(keep, x, 0.0)
        if b + 1 < nb:
            m = m[:, BK:] - dot_t(x, a_ref[hi:, lo:hi])


def factor(core, mine, other):
    vmem = pl.BlockSpec(memory_space=pltpu.VMEM)
    return pl.pallas_call(
        factor_kernel,
        out_shape=(jax.ShapeDtypeStruct((TOP, TOP), jnp.float32), jax.ShapeDtypeStruct((TOP, BK), jnp.float32)),
        in_specs=[pl.BlockSpec(memory_space=pltpu.SMEM), vmem, vmem],
        out_specs=(vmem, vmem),
    )(core, mine, other)


def solve(first, parts, low, inverses):
    vmem = pl.BlockSpec(memory_space=pltpu.VMEM)
    return pl.pallas_call(
        solve_kernel,
        out_shape=jax.ShapeDtypeStruct((parts[0].shape[0], TOP), jnp.float32),
        in_specs=[pl.BlockSpec(memory_space=pltpu.SMEM)] + [vmem] * 6,
        out_specs=vmem,
    )(first, *parts, low, inverses)


def shards(features, slab, pack_order, place_order, start):
    n_krow, n_col = lax.axis_size("krow"), lax.axis_size("col")
    rows_dev = features.shape[0]
    group = rows_dev // n_krow
    prior_dev = slab.shape[1]
    krow, col = lax.axis_index("krow"), lax.axis_index("col")

    kept = (col * prior_dev + jnp.arange(prior_dev) < start[0])[None, :]
    order = place_order[0]
    coded = jnp.stack([order // CODE, order % CODE], axis=1).astype(jnp.bfloat16)
    coded = jnp.pad(coded, ((0, 0), (0, BK - 2)))
    slab_part = swap(jnp.concatenate([slab, coded], axis=1), "krow")[:2 * group]
    packed = rows_at(features, pack_order[0])
    feat_dev = packed.shape[1]
    tiles = from_everyone(jnp.concatenate([packed[:2 * group], slab_part], axis=1), "krow")
    packed, tiles = lax.optimization_barrier((packed, tiles))
    arrived = swap(packed, "krow")

    tiles = tiles.reshape(n_krow, 2, group, tiles.shape[-1])
    top = jnp.moveaxis(tiles, 1, 0).reshape(TOP, tiles.shape[-1])
    places = top[:, feat_dev + prior_dev:feat_dev + prior_dev + 2].astype(jnp.float32).astype(jnp.int32)
    wanted = places[:, 0] * CODE + places[:, 1] + jnp.arange(TOP) // rows_dev * rows_dev
    top_feats = rows_at(top[:, :feat_dev], wanted)
    top_slab = jnp.where(kept, top[:, feat_dev:feat_dev + prior_dev], jnp.zeros((), jnp.bfloat16))
    top_norms = sq_norms(top_feats)

    share = PW // n_krow
    at = krow * share
    pair = at // BK
    row_lo = at
    row_hi = (7 - pair) * BK + (at - pair * BK)

    def rows_of(array, first):
        return lax.dynamic_slice_in_dim(array, first, share, 0)

    def both(array):
        return jnp.concatenate([rows_of(array, row_hi), rows_of(array, row_lo)], axis=0)

    gram = inner(both(top_feats), top_feats)
    dist = both(top_norms)[:, None] + top_norms[None, :] - 2.0 * gram
    update = inner(both(top_slab), top_slab)
    dist = fold(dist[:share], dist[share:], pair)
    update = fold(update[:share], update[share:], pair)
    parts = jnp.concatenate([dist, update], axis=1)
    parts, arrived = lax.optimization_barrier((parts, arrived))
    parts = swap(parts, "col")
    summed = jnp.sum(parts.reshape(n_col, share // n_col, 2 * 9 * BK), axis=0)
    dist, update = summed[:, :9 * BK], summed[:, 9 * BK:]
    mine = share // n_col
    col_ids = jnp.arange(TOP)[None, :]
    ids = jnp.arange(mine)[:, None] + col * mine
    shift = fold((row_hi + ids == col_ids).astype(jnp.float32),
                 (row_lo + ids == col_ids).astype(jnp.float32), pair)
    entries = jnp.exp(-dist / (2.0 * F)) + RIDGE * shift - update
    entries = from_everyone(entries, "col").reshape(share, 9 * BK)

    core, pair_at = col % 2, col // 2
    pairs = n_col // 2
    own = rows_dev // n_col

    def split_rows(array):
        array = array.reshape(pairs, 2, own, *array.shape[1:])
        halves = [lax.dynamic_index_in_dim(array, which, 1, keepdims=False) for which in (1 - core, core)]
        return jnp.concatenate([h.reshape(pairs * own, *h.shape[2:]) for h in halves], axis=0)

    ordered = rows_at(arrived, split_rows(place_order[0]))
    dist = sq_norms(ordered)[:, None] + top_norms[None, :] - 2.0 * inner(ordered, top_feats)
    update = inner(split_rows(slab), top_slab)
    parts = jnp.concatenate([dist, update], axis=1)
    half = pairs * own
    got = lax.ppermute(parts[:half], "col", [(c, c ^ 1) for c in range(n_col)])
    both_cores = (parts[half:] + got).reshape(pairs, own, 2 * TOP)
    both_cores, entries = lax.optimization_barrier((both_cores, entries))
    sums = [lax.dynamic_index_in_dim(both_cores, pair_at, 0, keepdims=False)]
    for away in range(1, pairs):
        piece = lax.dynamic_index_in_dim(both_cores, (pair_at + away) % pairs, 0, keepdims=False)
        to = [(c, (c // 2 + away) % pairs * 2 + c % 2) for c in range(n_col)]
        sums.append(lax.ppermute(piece, "col", to))

    half_share = share // 2
    piece = lax.dynamic_slice_in_dim(entries, core * half_share, half_share, 0)
    mine = from_everyone(piece, "krow")
    mine = mine.reshape(n_krow, half_share, 9 * BK)
    other = lax.ppermute(mine, "col", [(c, c ^ 1) for c in range(n_col)])
    low, inverses = factor(core.reshape(1), mine, other)
    first_row = krow * rows_dev + col * own
    return solve(first_row.reshape(1), sums, low, inverses)


def solution(mesh):
    in_specs = (P("krow", "col"), P("krow", "col"), P("krow", None), P("krow", None), P())
    out_specs = P(("krow", "col"), None)
    return jax.shard_map(shards, mesh=mesh, in_specs=in_specs, out_specs=out_specs, check_vma=False)
```

```python
import jax
import jax.numpy as jnp
from jax import lax
from jax.experimental import pallas as pl
from jax.experimental.pallas import tpu as pltpu
from jax.sharding import PartitionSpec as P

F = 6144
PW = 512
TOP = 2 * PW
BK = 128
CODE = 32
MB = 16
RIDGE = 0.5
HI = lax.Precision.HIGHEST


def rows_at(array, where):
    return array.at[where].get(mode="promise_in_bounds", unique_indices=True)


def swap(value, axis):
    return lax.all_to_all(value, axis, split_axis=0, concat_axis=0, tiled=True)


def from_everyone(value, axis):
    return swap(jnp.broadcast_to(value, (lax.axis_size(axis), *value.shape)), axis)


def sq_norms(rows):
    return jnp.sum(jnp.square(rows.astype(jnp.float32)), axis=1)


def inner(a, b):
    return lax.dot_general(a, b, (((1,), (1,)), ((), ())), preferred_element_type=jnp.float32)


def fold(upper, lower, pair):
    blocks = []
    for slot in range(9):
        hi = upper[:, slot * BK:(slot + 1) * BK] if slot < 8 else None
        at = 8 - slot
        lo = lower[:, at * BK:(at + 1) * BK] if slot > 4 else None
        if lo is None:
            blocks.append(hi)
        elif hi is None:
            blocks.append(lo)
        else:
            blocks.append(jnp.where(slot + pair <= 7, hi, lo))
    return jnp.concatenate(blocks, axis=1)


def dot_t(a, b):
    return lax.dot_general(a, b, (((1,), (1,)), ((), ())), precision=HI, preferred_element_type=jnp.float32)


def over_rows(v, k):
    return jnp.broadcast_to(v[k:k + 1, :], v.shape)


def over_lanes(v, c):
    return jnp.take_along_axis(v, jnp.full(v.shape, c, jnp.int32), axis=1, mode="promise_in_bounds")


def inverse_of(p):
    return 1.0 / p


def invert_factor(tiles, w_ref, first):
    n = len(tiles)
    lane = lax.broadcasted_iota(jnp.int32, (MB, BK), 1)
    sub = lax.broadcasted_iota(jnp.int32, (MB, BK), 0)
    for g in range(n):
        c0 = MB * g
        cols = [over_lanes(tiles[g], c0 + k) for k in range(MB)]
        own = (lane >= c0) & (lane < c0 + MB)
        both = jnp.where(own, jnp.where(lane == c0 + sub, 1.0, 0.0), tiles[g])
        down = both
        pivots = jnp.ones((MB, BK), jnp.float32)
        scale = pivots
        p = over_rows(cols[0], 0)
        for k in range(MB):
            r = inverse_of(p)
            pivots = jnp.where(sub == k, p, pivots)
            scale = jnp.where(sub == k, r, scale)
            if k + 1 < MB and 1:
                b = over_rows(cols[k], k + 1)
                p = over_rows(cols[k + 1], k + 1) - (b * b) * r
            m = jnp.where(sub == k, 0.0, cols[k] * r)
            row = over_rows(both, k)
            for k2 in range(k + 1, MB):
                cols[k2] = cols[k2] - m * over_rows(cols[k2], k)
            if k + 1 < MB and not 1:
                p = over_rows(cols[k + 1], k + 1)
            both = both - m * row
            down = down - jnp.where(sub > k, m, 0.0) * row
        w_ref[pl.ds(pl.multiple_of(first + c0, MB), MB), :] = (
            jnp.where(lane < c0 + MB, down, 0.0) * lax.rsqrt(pivots))
        both = both * scale
        rows = [over_rows(both, k) for k in range(MB)]
        for i in range(g + 1, n):
            tile = jnp.where(own, 0.0, tiles[i])
            for k in range(MB):
                tile = tile - over_lanes(tiles[i], c0 + k) * rows[k]
            tiles[i] = tile


def factor_kernel(core_ref, mine_ref, other_ref, a_ref, w_ref):
    nb = TOP // BK
    pieces = mine_ref.shape[0]
    half = mine_ref.shape[1]
    per = pieces // (nb // 2)

    def place(first, second):
        for b in range(nb // 2):
            for i in range(per):
                for h, ref in enumerate((first, second)):
                    src = ref[b * per + i]
                    at = i * 2 * half + h * half
                    r = nb - 1 - b
                    a_ref[r * BK + at:r * BK + at + half, :(r + 1) * BK] = src[:, :(r + 1) * BK]
                    for j in range(b + 1):
                        a_ref[b * BK + at:b * BK + at + half, j * BK:(j + 1) * BK] = (
                            src[:, (nb - j) * BK:(nb + 1 - j) * BK])

    @pl.when(core_ref[0] == 0)
    def _():
        place(mine_ref, other_ref)

    @pl.when(core_ref[0] != 0)
    def _():
        place(other_ref, mine_ref)

    def step(j, carry):
        o = pl.multiple_of(j * BK, BK)
        tiles = [a_ref[pl.ds(pl.multiple_of(o + MB * i, MB), MB), pl.ds(o, BK)] for i in range(BK // MB)]
        invert_factor(tiles, w_ref, o)
        for b in range(nb - 1):
            @pl.when(j == b)
            def _():
                lo, hi = b * BK, (b + 1) * BK
                panel = dot_t(a_ref[hi:, lo:hi], w_ref[lo:hi, :])
                a_ref[hi:, lo:hi] = panel
                for c in range(b + 1, nb):
                    at = c * BK
                    a_ref[at:, at:at + BK] -= dot_t(panel[at - hi:, :], panel[at - hi:at - hi + BK, :])
        return carry

    lax.fori_loop(0, nb, step, 0)


def solve_kernel(first_ref, d0_ref, d1_ref, d2_ref, d3_ref, u0_ref, u1_ref, u2_ref, u3_ref, a_ref, w_ref, o_ref):
    nb = TOP // BK
    dist = (d0_ref[...] + d1_ref[...]) + (d2_ref[...] + d3_ref[...])
    update = (u0_ref[...] + u1_ref[...]) + (u2_ref[...] + u3_ref[...])
    rows = dist.shape[0]
    pos = first_ref[0] + lax.broadcasted_iota(jnp.int32, (rows, TOP), 0)
    col = lax.broadcasted_iota(jnp.int32, (rows, TOP), 1)
    shift = jnp.where(pos == col, RIDGE, 0.0)
    m = jnp.exp(-dist / (2.0 * F)) + shift - update
    for b in range(nb):
        lo, hi = b * BK, (b + 1) * BK
        x = dot_t(m[:, :BK], w_ref[lo:hi, :])
        keep = (pos[:, lo:hi] >= PW) | (lo < PW)
        o_ref[:, lo:hi] = jnp.where(keep, x, 0.0)
        if b + 1 < nb:
            m = m[:, BK:] - dot_t(x, a_ref[hi:, lo:hi])


def factor(core, mine, other):
    vmem = pl.BlockSpec(memory_space=pltpu.VMEM)
    return pl.pallas_call(
        factor_kernel,
        out_shape=(jax.ShapeDtypeStruct((TOP, TOP), jnp.float32), jax.ShapeDtypeStruct((TOP, BK), jnp.float32)),
        in_specs=[pl.BlockSpec(memory_space=pltpu.SMEM), vmem, vmem],
        out_specs=(vmem, vmem),
    )(core, mine, other)


def solve(first, parts, low, inverses):
    vmem = pl.BlockSpec(memory_space=pltpu.VMEM)
    return pl.pallas_call(
        solve_kernel,
        out_shape=jax.ShapeDtypeStruct((parts[0].shape[0], TOP), jnp.float32),
        in_specs=[pl.BlockSpec(memory_space=pltpu.SMEM)] + [vmem] * (len(parts) + 2),
        out_specs=vmem,
    )(first, *parts, low, inverses)


def shards(features, slab, pack_order, place_order, start):
    n_krow, n_col = lax.axis_size("krow"), lax.axis_size("col")
    rows_dev = features.shape[0]
    group = rows_dev // n_krow
    prior_dev = slab.shape[1]
    krow, col = lax.axis_index("krow"), lax.axis_index("col")

    kept = (col * prior_dev + jnp.arange(prior_dev) < start[0])[None, :]
    order = place_order[0]
    coded = jnp.stack([order // CODE, order % CODE], axis=1).astype(jnp.bfloat16)
    coded = jnp.pad(coded, ((0, 0), (0, BK - 2)))
    slab_part = swap(jnp.concatenate([slab, coded], axis=1), "krow")[:2 * group]
    packed = rows_at(features, pack_order[0])
    feat_dev = packed.shape[1]
    tiles = from_everyone(jnp.concatenate([packed[:2 * group], slab_part], axis=1), "krow")
    packed, tiles = lax.optimization_barrier((packed, tiles))
    arrived = swap(packed, "krow")

    tiles = tiles.reshape(n_krow, 2, group, tiles.shape[-1])
    top = jnp.moveaxis(tiles, 1, 0).reshape(TOP, tiles.shape[-1])
    places = top[:, feat_dev + prior_dev:feat_dev + prior_dev + 2].astype(jnp.float32).astype(jnp.int32)
    wanted = (places[:, :1] * CODE + places[:, 1:]).reshape(2, rows_dev, 1)
    pick = (wanted == jnp.arange(rows_dev)).astype(jnp.bfloat16)
    top_feats = jnp.einsum("bij,bjf->bif", pick, top[:, :feat_dev].reshape(2, rows_dev, feat_dev),
                           preferred_element_type=jnp.float32).astype(jnp.bfloat16).reshape(TOP, feat_dev)
    top_slab = jnp.where(kept, top[:, feat_dev:feat_dev + prior_dev], jnp.zeros((), jnp.bfloat16))
    top_norms = sq_norms(top_feats)

    share = PW // n_krow
    at = krow * share
    pair = at // BK
    row_lo = at
    row_hi = (7 - pair) * BK + (at - pair * BK)

    def rows_of(array, first):
        return lax.dynamic_slice_in_dim(array, first, share, 0)

    def both(array):
        return jnp.concatenate([rows_of(array, row_hi), rows_of(array, row_lo)], axis=0)

    gram = inner(both(top_feats), top_feats)
    dist = both(top_norms)[:, None] + top_norms[None, :] - 2.0 * gram
    update = inner(both(top_slab), top_slab)
    dist = fold(dist[:share], dist[share:], pair)
    update = fold(update[:share], update[share:], pair)
    parts = jnp.concatenate([dist, update], axis=1)
    parts, arrived = lax.optimization_barrier((parts, arrived))
    parts = swap(parts, "col")
    summed = jnp.sum(parts.reshape(n_col, share // n_col, 2 * 9 * BK), axis=0)
    dist, update = summed[:, :9 * BK], summed[:, 9 * BK:]
    mine = share // n_col
    col_ids = jnp.arange(TOP)[None, :]
    ids = jnp.arange(mine)[:, None] + col * mine
    shift = fold((row_hi + ids == col_ids).astype(jnp.float32),
                 (row_lo + ids == col_ids).astype(jnp.float32), pair)
    entries = jnp.exp(-dist / (2.0 * F)) + RIDGE * shift - update
    entries = from_everyone(entries, "col").reshape(share, 9 * BK)

    core, pair_at = col % 2, col // 2
    pairs = n_col // 2
    own = rows_dev // n_col

    def split_rows(array):
        array = array.reshape(pairs, 2, own, *array.shape[1:])
        halves = [lax.dynamic_index_in_dim(array, which, 1, keepdims=False) for which in (1 - core, core)]
        return jnp.concatenate([h.reshape(pairs * own, *h.shape[2:]) for h in halves], axis=0)

    def other_core(value):
        return lax.ppermute(value, "col", [(c, c ^ 1) for c in range(n_col)])

    def spread_over_pairs(value):
        pieces = [lax.dynamic_index_in_dim(value, pair_at, 0, keepdims=False)]
        for away in range(1, pairs):
            piece = lax.dynamic_index_in_dim(value, (pair_at + away) % pairs, 0, keepdims=False)
            to = [(c, (c // 2 + away) % pairs * 2 + c % 2) for c in range(n_col)]
            pieces.append(lax.ppermute(piece, "col", to))
        return pieces

    half = pairs * own
    update = inner(split_rows(slab), top_slab)
    updates = (update[half:] + other_core(update[:half])).reshape(pairs, own, TOP)
    updates = spread_over_pairs(updates)

    ordered = rows_at(arrived, split_rows(place_order[0]))
    dist = sq_norms(ordered)[:, None] + top_norms[None, :] - 2.0 * inner(ordered, top_feats)
    dists = (dist[half:] + other_core(dist[:half])).reshape(pairs, own, TOP)
    dists, entries = lax.optimization_barrier((dists, entries))
    dists = spread_over_pairs(dists)

    half_share = share // 2
    piece = lax.dynamic_slice_in_dim(entries, core * half_share, half_share, 0)
    mine = from_everyone(piece, "krow")
    mine = mine.reshape(n_krow, half_share, 9 * BK)
    other = lax.ppermute(mine, "col", [(c, c ^ 1) for c in range(n_col)])
    low, inverses = factor(core.reshape(1), mine, other)
    first_row = krow * rows_dev + col * own
    return solve(first_row.reshape(1), dists + updates, low, inverses)


def solution(mesh):
    in_specs = (P("krow", "col"), P("krow", "col"), P("krow", None), P("krow", None), P())
    out_specs = P(("krow", "col"), None)
    return jax.shard_map(shards, mesh=mesh, in_specs=in_specs, out_specs=out_specs, check_vma=False)
```

```python
import jax
import jax.numpy as jnp
from jax import lax
from jax.experimental import pallas as pl
from jax.experimental.pallas import tpu as pltpu
from jax.sharding import PartitionSpec as P

F = 6144
PW = 512
TOP = 2 * PW
BK = 128
CODE = 32
MB = 16
RIDGE = 0.5
HI = lax.Precision.HIGHEST


def rows_at(array, where):
    return array.at[where].get(mode="promise_in_bounds", unique_indices=True)


def swap(value, axis):
    return lax.all_to_all(value, axis, split_axis=0, concat_axis=0, tiled=True)


def from_everyone(value, axis):
    return swap(jnp.broadcast_to(value, (lax.axis_size(axis), *value.shape)), axis)


def sq_norms(rows):
    return jnp.sum(jnp.square(rows.astype(jnp.float32)), axis=1)


def inner(a, b):
    return lax.dot_general(a, b, (((1,), (1,)), ((), ())), preferred_element_type=jnp.float32)


def fold(upper, lower, pair):
    blocks = []
    for slot in range(9):
        hi = upper[:, slot * BK:(slot + 1) * BK] if slot < 8 else None
        at = 8 - slot
        lo = lower[:, at * BK:(at + 1) * BK] if slot > 4 else None
        if lo is None:
            blocks.append(hi)
        elif hi is None:
            blocks.append(lo)
        else:
            blocks.append(jnp.where(slot + pair <= 7, hi, lo))
    return jnp.concatenate(blocks, axis=1)


def dot_t(a, b):
    return lax.dot_general(a, b, (((1,), (1,)), ((), ())), precision=HI, preferred_element_type=jnp.float32)


def over_rows(v, k):
    return jnp.broadcast_to(v[k:k + 1, :], v.shape)


def over_lanes(v, c):
    return jnp.take_along_axis(v, jnp.full(v.shape, c, jnp.int32), axis=1, mode="promise_in_bounds")


def inverse_of(p):
    return 1.0 / p


def invert_factor(tiles, w_ref, first):
    n = len(tiles)
    lane = lax.broadcasted_iota(jnp.int32, (MB, BK), 1)
    sub = lax.broadcasted_iota(jnp.int32, (MB, BK), 0)
    for g in range(n):
        c0 = MB * g
        cols = [over_lanes(tiles[g], c0 + k) for k in range(MB)]
        own = (lane >= c0) & (lane < c0 + MB)
        both = jnp.where(own, jnp.where(lane == c0 + sub, 1.0, 0.0), tiles[g])
        down = both
        pivots = jnp.ones((MB, BK), jnp.float32)
        scale = pivots
        p = over_rows(cols[0], 0)
        for k in range(MB):
            r = inverse_of(p)
            pivots = jnp.where(sub == k, p, pivots)
            scale = jnp.where(sub == k, r, scale)
            if k + 1 < MB and 1:
                b = over_rows(cols[k], k + 1)
                p = over_rows(cols[k + 1], k + 1) - (b * b) * r
            m = jnp.where(sub == k, 0.0, cols[k] * r)
            row = over_rows(both, k)
            for k2 in range(k + 1, MB):
                cols[k2] = cols[k2] - m * over_rows(cols[k2], k)
            if k + 1 < MB and not 1:
                p = over_rows(cols[k + 1], k + 1)
            both = both - m * row
            down = down - jnp.where(sub > k, m, 0.0) * row
        w_ref[pl.ds(pl.multiple_of(first + c0, MB), MB), :] = (
            jnp.where(lane < c0 + MB, down, 0.0) * lax.rsqrt(pivots))
        both = both * scale
        rows = [over_rows(both, k) for k in range(MB)]
        for i in range(g + 1, n):
            tile = jnp.where(own, 0.0, tiles[i])
            for k in range(MB):
                tile = tile - over_lanes(tiles[i], c0 + k) * rows[k]
            tiles[i] = tile


def factor_kernel(core_ref, mine_ref, other_ref, a_ref, w_ref):
    nb = TOP // BK
    pieces = mine_ref.shape[0]
    half = mine_ref.shape[1]
    per = pieces // (nb // 2)

    def place(first, second):
        for b in range(nb // 2):
            for i in range(per):
                for h, ref in enumerate((first, second)):
                    src = ref[b * per + i]
                    at = i * 2 * half + h * half
                    r = nb - 1 - b
                    a_ref[r * BK + at:r * BK + at + half, :(r + 1) * BK] = src[:, :(r + 1) * BK]
                    for j in range(b + 1):
                        a_ref[b * BK + at:b * BK + at + half, j * BK:(j + 1) * BK] = (
                            src[:, (nb - j) * BK:(nb + 1 - j) * BK])

    @pl.when(core_ref[0] == 0)
    def _():
        place(mine_ref, other_ref)

    @pl.when(core_ref[0] != 0)
    def _():
        place(other_ref, mine_ref)

    def step(j, carry):
        o = pl.multiple_of(j * BK, BK)
        tiles = [a_ref[pl.ds(pl.multiple_of(o + MB * i, MB), MB), pl.ds(o, BK)] for i in range(BK // MB)]
        invert_factor(tiles, w_ref, o)
        for b in range(nb - 1):
            @pl.when(j == b)
            def _():
                lo, hi = b * BK, (b + 1) * BK
                panel = dot_t(a_ref[hi:, lo:hi], w_ref[lo:hi, :])
                a_ref[hi:, lo:hi] = panel
                for c in range(b + 1, nb):
                    at = c * BK
                    a_ref[at:, at:at + BK] -= dot_t(panel[at - hi:, :], panel[at - hi:at - hi + BK, :])
        return carry

    lax.fori_loop(0, nb, step, 0)


def solve_kernel(first_ref, d0_ref, d1_ref, d2_ref, d3_ref, u0_ref, u1_ref, u2_ref, u3_ref, a_ref, w_ref, o_ref):
    nb = TOP // BK
    dist = (d0_ref[...] + d1_ref[...]) + (d2_ref[...] + d3_ref[...])
    update = (u0_ref[...] + u1_ref[...]) + (u2_ref[...] + u3_ref[...])
    rows = dist.shape[0]
    pos = first_ref[0] + lax.broadcasted_iota(jnp.int32, (rows, TOP), 0)
    col = lax.broadcasted_iota(jnp.int32, (rows, TOP), 1)
    shift = jnp.where(pos == col, RIDGE, 0.0)
    m = jnp.exp(-dist / (2.0 * F)) + shift - update
    for b in range(nb):
        lo, hi = b * BK, (b + 1) * BK
        x = dot_t(m[:, :BK], w_ref[lo:hi, :])
        keep = (pos[:, lo:hi] >= PW) | (lo < PW)
        o_ref[:, lo:hi] = jnp.where(keep, x, 0.0)
        if b + 1 < nb:
            m = m[:, BK:] - dot_t(x, a_ref[hi:, lo:hi])


def factor(core, mine, other):
    vmem = pl.BlockSpec(memory_space=pltpu.VMEM)
    return pl.pallas_call(
        factor_kernel,
        out_shape=(jax.ShapeDtypeStruct((TOP, TOP), jnp.float32), jax.ShapeDtypeStruct((TOP, BK), jnp.float32)),
        in_specs=[pl.BlockSpec(memory_space=pltpu.SMEM), vmem, vmem],
        out_specs=(vmem, vmem),
    )(core, mine, other)


def solve(first, parts, low, inverses):
    vmem = pl.BlockSpec(memory_space=pltpu.VMEM)
    return pl.pallas_call(
        solve_kernel,
        out_shape=jax.ShapeDtypeStruct((parts[0].shape[0], TOP), jnp.float32),
        in_specs=[pl.BlockSpec(memory_space=pltpu.SMEM)] + [vmem] * (len(parts) + 2),
        out_specs=vmem,
    )(first, *parts, low, inverses)


def shards(features, slab, pack_order, place_order, start):
    n_krow, n_col = lax.axis_size("krow"), lax.axis_size("col")
    rows_dev = features.shape[0]
    group = rows_dev // n_krow
    prior_dev = slab.shape[1]
    krow, col = lax.axis_index("krow"), lax.axis_index("col")

    kept = (col * prior_dev + jnp.arange(prior_dev) < start[0])[None, :]
    order = place_order[0]
    coded = jnp.stack([order // CODE, order % CODE], axis=1).astype(jnp.bfloat16)
    coded = jnp.pad(coded, ((0, 0), (0, BK - 2)))
    packed = rows_at(features, pack_order[0])
    feat_dev = packed.shape[1]
    arrived = swap(jnp.concatenate([packed, slab, coded], axis=1), "krow")
    mine = jnp.concatenate([packed[:2 * group], arrived[:2 * group, feat_dev:]], axis=1)
    arrived = arrived[:, :feat_dev]
    tiles = from_everyone(mine, "krow")

    tiles = tiles.reshape(n_krow, 2, group, tiles.shape[-1])
    top = jnp.moveaxis(tiles, 1, 0).reshape(TOP, tiles.shape[-1])
    places = top[:, feat_dev + prior_dev:feat_dev + prior_dev + 2].astype(jnp.float32).astype(jnp.int32)
    wanted = (places[:, :1] * CODE + places[:, 1:]).reshape(2, rows_dev, 1)
    pick = (wanted == jnp.arange(rows_dev)).astype(jnp.bfloat16)
    top_feats = jnp.einsum("bij,bjf->bif", pick, top[:, :feat_dev].reshape(2, rows_dev, feat_dev),
                           preferred_element_type=jnp.float32).astype(jnp.bfloat16).reshape(TOP, feat_dev)
    top_slab = jnp.where(kept, top[:, feat_dev:feat_dev + prior_dev], jnp.zeros((), jnp.bfloat16))
    top_norms = sq_norms(top_feats)

    share = PW // n_krow
    at = krow * share
    pair = at // BK
    row_lo = at
    row_hi = (7 - pair) * BK + (at - pair * BK)

    def rows_of(array, first):
        return lax.dynamic_slice_in_dim(array, first, share, 0)

    def both(array):
        return jnp.concatenate([rows_of(array, row_hi), rows_of(array, row_lo)], axis=0)

    gram = inner(both(top_feats), top_feats)
    dist = both(top_norms)[:, None] + top_norms[None, :] - 2.0 * gram
    update = inner(both(top_slab), top_slab)
    dist = fold(dist[:share], dist[share:], pair)
    update = fold(update[:share], update[share:], pair)
    parts = jnp.concatenate([dist, update], axis=1)
    parts = swap(parts, "col")
    summed = jnp.sum(parts.reshape(n_col, share // n_col, 2 * 9 * BK), axis=0)
    dist, update = summed[:, :9 * BK], summed[:, 9 * BK:]
    mine = share // n_col
    col_ids = jnp.arange(TOP)[None, :]
    ids = jnp.arange(mine)[:, None] + col * mine
    shift = fold((row_hi + ids == col_ids).astype(jnp.float32),
                 (row_lo + ids == col_ids).astype(jnp.float32), pair)
    entries = jnp.exp(-dist / (2.0 * F)) + RIDGE * shift - update
    entries = from_everyone(entries, "col")
    entries = entries.reshape(share, 9 * BK)

    core, pair_at = col % 2, col // 2
    pairs = n_col // 2
    own = rows_dev // n_col

    def split_rows(array):
        array = array.reshape(pairs, 2, own, *array.shape[1:])
        halves = [lax.dynamic_index_in_dim(array, which, 1, keepdims=False) for which in (1 - core, core)]
        return jnp.concatenate([h.reshape(pairs * own, *h.shape[2:]) for h in halves], axis=0)

    def other_core(value):
        return lax.ppermute(value, "col", [(c, c ^ 1) for c in range(n_col)])

    def spread_over_pairs(value):
        pieces = [lax.dynamic_index_in_dim(value, pair_at, 0, keepdims=False)]
        for away in range(1, pairs):
            piece = lax.dynamic_index_in_dim(value, (pair_at + away) % pairs, 0, keepdims=False)
            to = [(c, (c // 2 + away) % pairs * 2 + c % 2) for c in range(n_col)]
            pieces.append(lax.ppermute(piece, "col", to))
        return pieces

    half = pairs * own
    update = inner(split_rows(slab), top_slab)
    updates = (update[half:] + other_core(update[:half])).reshape(pairs, own, TOP)
    updates = spread_over_pairs(updates)

    ordered = rows_at(arrived, split_rows(place_order[0]))
    dist = sq_norms(ordered)[:, None] + top_norms[None, :] - 2.0 * inner(ordered, top_feats)
    dists = (dist[half:] + other_core(dist[:half])).reshape(pairs, own, TOP)
    dists = spread_over_pairs(dists)

    half_share = share // 2
    piece = lax.dynamic_slice_in_dim(entries, core * half_share, half_share, 0)
    mine = from_everyone(piece, "krow")
    mine = mine.reshape(n_krow, half_share, 9 * BK)
    other = lax.ppermute(mine, "col", [(c, c ^ 1) for c in range(n_col)])
    low, inverses = factor(core.reshape(1), mine, other)
    first_row = krow * rows_dev + col * own
    return solve(first_row.reshape(1), dists + updates, low, inverses)


def solution(mesh):
    in_specs = (P("krow", "col"), P("krow", "col"), P("krow", None), P("krow", None), P())
    out_specs = P(("krow", "col"), None)
    return jax.shard_map(shards, mesh=mesh, in_specs=in_specs, out_specs=out_specs, check_vma=False)
```

```python
import jax
import jax.numpy as jnp
from jax import lax
from jax.experimental import pallas as pl
from jax.experimental.pallas import tpu as pltpu
from jax.sharding import PartitionSpec as P

F = 6144
PW = 512
TOP = 2 * PW
BK = 128
CODE = 32
MB = 16
RIDGE = 0.5


def rows_at(array, where):
    dims = lax.GatherDimensionNumbers(offset_dims=(1,), collapsed_slice_dims=(0,), start_index_map=(0,))
    return lax.gather(array, where[:, None], dims, (1, array.shape[1]), unique_indices=True,
                      mode=lax.GatherScatterMode.PROMISE_IN_BOUNDS)


def swap(value, axis):
    return lax.all_to_all(value, axis, split_axis=0, concat_axis=0, tiled=True)


def from_everyone(value, axis):
    return swap(jnp.broadcast_to(value, (lax.axis_size(axis), *value.shape)), axis)


def sq_norms(rows):
    return jnp.sum(jnp.square(rows.astype(jnp.float32)), axis=1)


def inner(a, b):
    return lax.dot_general(a, b, (((1,), (1,)), ((), ())), preferred_element_type=jnp.float32)


def fold(upper, lower, pair):
    blocks = []
    for slot in range(9):
        hi = upper[:, slot * BK:(slot + 1) * BK] if slot < 8 else None
        at = 8 - slot
        lo = lower[:, at * BK:(at + 1) * BK] if slot > 4 else None
        if lo is None:
            blocks.append(hi)
        elif hi is None:
            blocks.append(lo)
        else:
            blocks.append(jnp.where(slot + pair <= 7, hi, lo))
    return jnp.concatenate(blocks, axis=1)


def parts_of(x):
    high = x.astype(jnp.bfloat16)
    rest = x - high.astype(jnp.float32)
    mid = rest.astype(jnp.bfloat16)
    low = (rest - mid.astype(jnp.float32)).astype(jnp.bfloat16)
    return high, mid, low


def left(x):
    h, m, l = parts_of(x)
    return jnp.concatenate([h, h, m, m, h, l], axis=1)


def right(x):
    h, m, l = parts_of(x)
    return jnp.concatenate([h, m, h, m, l, h], axis=1)


def long_dot(a, b):
    return lax.dot_general(a, b, (((1,), (1,)), ((), ())), preferred_element_type=jnp.float32)


def over_rows(v, k):
    return jnp.broadcast_to(v[k:k + 1, :], v.shape)


def over_lanes(v, c):
    return jnp.take_along_axis(v, jnp.full(v.shape, c, jnp.int32), axis=1, mode="promise_in_bounds")


def inverse_of(p):
    return 1.0 / p


def invert_factor(tiles, w_ref, first):
    n = len(tiles)
    lane = lax.broadcasted_iota(jnp.int32, (MB, BK), 1)
    sub = lax.broadcasted_iota(jnp.int32, (MB, BK), 0)
    for g in range(n):
        c0 = MB * g
        cols = [over_lanes(tiles[g], c0 + k) for k in range(MB)]
        own = (lane >= c0) & (lane < c0 + MB)
        both = jnp.where(own, jnp.where(lane == c0 + sub, 1.0, 0.0), tiles[g])
        down = both
        pivots = jnp.ones((MB, BK), jnp.float32)
        scale = pivots
        p = over_rows(cols[0], 0)
        for k in range(MB):
            r = inverse_of(p)
            pivots = jnp.where(sub == k, p, pivots)
            scale = jnp.where(sub == k, r, scale)
            if k + 1 < MB and 1:
                b = over_rows(cols[k], k + 1)
                p = over_rows(cols[k + 1], k + 1) - (b * b) * r
            m = jnp.where(sub == k, 0.0, cols[k] * r)
            row = over_rows(both, k)
            for k2 in range(k + 1, MB):
                cols[k2] = cols[k2] - m * over_rows(cols[k2], k)
            if k + 1 < MB and not 1:
                p = over_rows(cols[k + 1], k + 1)
            both = both - m * row
            down = down - jnp.where(sub > k, m, 0.0) * row
        w_ref[pl.ds(pl.multiple_of(first + c0, MB), MB), :] = (
            jnp.where(lane < c0 + MB, down, 0.0) * lax.rsqrt(pivots))
        both = both * scale
        rows = [over_rows(both, k) for k in range(MB)]
        for i in range(g + 1, n):
            tile = jnp.where(own, 0.0, tiles[i])
            for k in range(MB):
                tile = tile - over_lanes(tiles[i], c0 + k) * rows[k]
            tiles[i] = tile


def factor_kernel(core_ref, mine_ref, other_ref, a_ref, w_ref):
    nb = TOP // BK
    pieces = mine_ref.shape[0]
    half = mine_ref.shape[1]
    per = pieces // (nb // 2)

    def place(first, second):
        for b in range(nb // 2):
            for i in range(per):
                for h, ref in enumerate((first, second)):
                    src = ref[b * per + i]
                    at = i * 2 * half + h * half
                    r = nb - 1 - b
                    a_ref[r * BK + at:r * BK + at + half, :(r + 1) * BK] = src[:, :(r + 1) * BK]
                    for j in range(b + 1):
                        a_ref[b * BK + at:b * BK + at + half, j * BK:(j + 1) * BK] = (
                            src[:, (nb - j) * BK:(nb + 1 - j) * BK])

    @pl.when(core_ref[0] == 0)
    def _():
        place(mine_ref, other_ref)

    @pl.when(core_ref[0] != 0)
    def _():
        place(other_ref, mine_ref)

    def step(j, carry):
        o = pl.multiple_of(j * BK, BK)
        tiles = [a_ref[pl.ds(pl.multiple_of(o + MB * i, MB), MB), pl.ds(o, BK)] for i in range(BK // MB)]
        invert_factor(tiles, w_ref, o)
        for b in range(nb - 1):
            @pl.when(j == b)
            def _():
                lo, hi = b * BK, (b + 1) * BK
                panel = long_dot(left(a_ref[hi:, lo:hi]), right(w_ref[lo:hi, :]))
                a_ref[hi:, lo:hi] = panel
                pl_, pr_ = left(panel), right(panel)
                for at in range(hi, TOP, 256):
                    to = min(at + 256, TOP)
                    a_ref[at:, at:to] -= long_dot(pl_[at - hi:], pr_[at - hi:to - hi])
        return carry

    lax.fori_loop(0, nb, step, 0)


def solve_kernel(first_ref, d0_ref, d1_ref, d2_ref, d3_ref, u0_ref, u1_ref, u2_ref, u3_ref, a_ref, w_ref, o_ref):
    nb = TOP // BK
    dist = (d0_ref[...] + d1_ref[...]) + (d2_ref[...] + d3_ref[...])
    update = (u0_ref[...] + u1_ref[...]) + (u2_ref[...] + u3_ref[...])
    rows = dist.shape[0]
    pos = first_ref[0] + lax.broadcasted_iota(jnp.int32, (rows, TOP), 0)
    col = lax.broadcasted_iota(jnp.int32, (rows, TOP), 1)
    shift = jnp.where(pos == col, RIDGE, 0.0)
    m = jnp.exp(-dist / (2.0 * F)) + shift - update
    for b in range(nb):
        lo, hi = b * BK, (b + 1) * BK
        x = long_dot(left(m[:, :BK]), right(w_ref[lo:hi, :]))
        keep = (pos[:, lo:hi] >= PW) | (lo < PW)
        o_ref[:, lo:hi] = jnp.where(keep, x, 0.0)
        if b + 1 < nb:
            m = m[:, BK:] - long_dot(left(x), right(a_ref[hi:, lo:hi]))


def factor(core, mine, other):
    vmem = pl.BlockSpec(memory_space=pltpu.VMEM)
    return pl.pallas_call(
        factor_kernel,
        out_shape=(jax.ShapeDtypeStruct((TOP, TOP), jnp.float32), jax.ShapeDtypeStruct((TOP, BK), jnp.float32)),
        in_specs=[pl.BlockSpec(memory_space=pltpu.SMEM), vmem, vmem],
        out_specs=(vmem, vmem),
    )(core, mine, other)


def solve(first, parts, low, inverses):
    vmem = pl.BlockSpec(memory_space=pltpu.VMEM)
    return pl.pallas_call(
        solve_kernel,
        out_shape=jax.ShapeDtypeStruct((parts[0].shape[0], TOP), jnp.float32),
        in_specs=[pl.BlockSpec(memory_space=pltpu.SMEM)] + [vmem] * (len(parts) + 2),
        out_specs=vmem,
    )(first, *parts, low, inverses)


def shards(features, slab, pack_order, place_order, start):
    n_krow, n_col = lax.axis_size("krow"), lax.axis_size("col")
    rows_dev = features.shape[0]
    group = rows_dev // n_krow
    prior_dev = slab.shape[1]
    krow, col = lax.axis_index("krow"), lax.axis_index("col")

    kept = (col * prior_dev + jnp.arange(prior_dev) < start[0])[None, :]
    order = place_order[0]
    coded = jnp.stack([order // CODE, order % CODE], axis=1).astype(jnp.bfloat16)
    coded = jnp.pad(coded, ((0, 0), (0, BK - 2)))
    packed = rows_at(features, pack_order[0])
    feat_dev = packed.shape[1]
    arrived = swap(jnp.concatenate([packed, slab, coded], axis=1), "krow")
    mine = jnp.concatenate([packed[:2 * group], arrived[:2 * group, feat_dev:]], axis=1)
    arrived = arrived[:, :feat_dev]
    tiles = from_everyone(mine, "krow")

    tiles = tiles.reshape(n_krow, 2, group, tiles.shape[-1])
    top = jnp.moveaxis(tiles, 1, 0).reshape(TOP, tiles.shape[-1])
    places = top[:, feat_dev + prior_dev:feat_dev + prior_dev + 2].astype(jnp.float32).astype(jnp.int32)
    wanted = (places[:, :1] * CODE + places[:, 1:]).reshape(2, rows_dev, 1)
    pick = (wanted == jnp.arange(rows_dev)).astype(jnp.bfloat16)
    top_feats = jnp.einsum("bij,bjf->bif", pick, top[:, :feat_dev].reshape(2, rows_dev, feat_dev),
                           preferred_element_type=jnp.float32).astype(jnp.bfloat16).reshape(TOP, feat_dev)
    top_slab = jnp.where(kept, top[:, feat_dev:feat_dev + prior_dev], jnp.zeros((), jnp.bfloat16))
    top_norms = sq_norms(top_feats)

    share = PW // n_krow
    at = krow * share
    pair = at // BK
    row_lo = at
    row_hi = (7 - pair) * BK + (at - pair * BK)

    def rows_of(array, first):
        return lax.dynamic_slice_in_dim(array, first, share, 0)

    def both(array):
        return jnp.concatenate([rows_of(array, row_hi), rows_of(array, row_lo)], axis=0)

    gram = inner(both(top_feats), top_feats)
    dist = both(top_norms)[:, None] + top_norms[None, :] - 2.0 * gram
    update = inner(both(top_slab), top_slab)
    dist = fold(dist[:share], dist[share:], pair)
    update = fold(update[:share], update[share:], pair)
    parts = jnp.concatenate([dist, update], axis=1)
    parts = swap(parts, "col")
    summed = jnp.sum(parts.reshape(n_col, share // n_col, 2 * 9 * BK), axis=0)
    dist, update = summed[:, :9 * BK], summed[:, 9 * BK:]
    mine = share // n_col
    col_ids = jnp.arange(TOP)[None, :]
    ids = jnp.arange(mine)[:, None] + col * mine
    shift = fold((row_hi + ids == col_ids).astype(jnp.float32),
                 (row_lo + ids == col_ids).astype(jnp.float32), pair)
    entries = jnp.exp(-dist / (2.0 * F)) + RIDGE * shift - update
    entries = from_everyone(entries, "col")
    entries = entries.reshape(share, 9 * BK)

    core, pair_at = col % 2, col // 2
    pairs = n_col // 2
    own = rows_dev // n_col

    def split_rows(array):
        array = array.reshape(pairs, 2, own, *array.shape[1:])
        halves = [lax.dynamic_index_in_dim(array, which, 1, keepdims=False) for which in (1 - core, core)]
        return jnp.concatenate([h.reshape(pairs * own, *h.shape[2:]) for h in halves], axis=0)

    def other_core(value):
        return lax.ppermute(value, "col", [(c, c ^ 1) for c in range(n_col)])

    def spread_over_pairs(value):
        pieces = [lax.dynamic_index_in_dim(value, pair_at, 0, keepdims=False)]
        for away in range(1, pairs):
            piece = lax.dynamic_index_in_dim(value, (pair_at + away) % pairs, 0, keepdims=False)
            to = [(c, (c // 2 + away) % pairs * 2 + c % 2) for c in range(n_col)]
            pieces.append(lax.ppermute(piece, "col", to))
        return pieces

    half = pairs * own
    update = inner(split_rows(slab), top_slab)
    update_got = other_core(update[:half])
    updates = (update[half:] + update_got).reshape(pairs, own, TOP)
    updates = spread_over_pairs(updates)

    ordered = rows_at(arrived, split_rows(place_order[0]))
    dist = sq_norms(ordered)[:, None] + top_norms[None, :] - 2.0 * inner(ordered, top_feats)
    dist_got = other_core(dist[:half])
    dists = (dist[half:] + dist_got).reshape(pairs, own, TOP)
    dists = spread_over_pairs(dists)

    half_share = share // 2
    piece = lax.dynamic_slice_in_dim(entries, core * half_share, half_share, 0)
    mine = from_everyone(piece, "krow")
    mine = mine.reshape(n_krow, half_share, 9 * BK)
    other = lax.ppermute(mine, "col", [(c, c ^ 1) for c in range(n_col)])
    low, inverses = factor(core.reshape(1), mine, other)
    first_row = krow * rows_dev + col * own
    return solve(first_row.reshape(1), dists + updates, low, inverses)


def solution(mesh):
    in_specs = (P("krow", "col"), P("krow", "col"), P("krow", None), P("krow", None), P())
    out_specs = P(("krow", "col"), None)
    return jax.shard_map(shards, mesh=mesh, in_specs=in_specs, out_specs=out_specs, check_vma=False)
```

```python
import jax
import jax.numpy as jnp
from jax import lax
from jax.experimental import pallas as pl
from jax.experimental.pallas import tpu as pltpu
from jax.sharding import PartitionSpec as P

F = 6144
PW = 512
TOP = 2 * PW
BK = 128
CODE = 32
MB = 16
RIDGE = 0.5


def rows_at(array, where):
    dims = lax.GatherDimensionNumbers(offset_dims=(1,), collapsed_slice_dims=(0,), start_index_map=(0,))
    return lax.gather(array, where[:, None], dims, (1, array.shape[1]), unique_indices=True,
                      mode=lax.GatherScatterMode.PROMISE_IN_BOUNDS)


def swap(value, axis):
    return lax.all_to_all(value, axis, split_axis=0, concat_axis=0, tiled=True)


def from_everyone(value, axis):
    return swap(jnp.broadcast_to(value, (lax.axis_size(axis), *value.shape)), axis)


def sq_norms(rows):
    return jnp.sum(jnp.square(rows.astype(jnp.float32)), axis=1)


def inner(a, b):
    return lax.dot_general(a, b, (((1,), (1,)), ((), ())), preferred_element_type=jnp.float32)


def fold(upper, lower, pair):
    blocks = []
    for slot in range(9):
        hi = upper[:, slot * BK:(slot + 1) * BK] if slot < 8 else None
        at = 8 - slot
        lo = lower[:, at * BK:(at + 1) * BK] if slot > 4 else None
        if lo is None:
            blocks.append(hi)
        elif hi is None:
            blocks.append(lo)
        else:
            blocks.append(jnp.where(slot + pair <= 7, hi, lo))
    return jnp.concatenate(blocks, axis=1)


def parts_of(x):
    high = x.astype(jnp.bfloat16)
    rest = x - high.astype(jnp.float32)
    mid = rest.astype(jnp.bfloat16)
    low = (rest - mid.astype(jnp.float32)).astype(jnp.bfloat16)
    return high, mid, low


def left(x):
    h, m, l = parts_of(x)
    return jnp.concatenate([h, h, m, m, h, l], axis=1)


def right(x):
    h, m, l = parts_of(x)
    return jnp.concatenate([h, m, h, m, l, h], axis=1)


def long_dot(a, b):
    return lax.dot_general(a, b, (((1,), (1,)), ((), ())), preferred_element_type=jnp.float32)


def over_rows(v, k):
    return jnp.broadcast_to(v[k:k + 1, :], v.shape)


def over_lanes(v, c):
    return jnp.take_along_axis(v, jnp.full(v.shape, c, jnp.int32), axis=1, mode="promise_in_bounds")


def inverse_of(p):
    return 1.0 / p


def invert_factor(tiles, w_ref, first):
    n = len(tiles)
    lane = lax.broadcasted_iota(jnp.int32, (MB, BK), 1)
    sub = lax.broadcasted_iota(jnp.int32, (MB, BK), 0)
    for g in range(n):
        c0 = MB * g
        cols = [over_lanes(tiles[g], c0 + k) for k in range(MB)]
        own = (lane >= c0) & (lane < c0 + MB)
        both = jnp.where(own, jnp.where(lane == c0 + sub, 1.0, 0.0), tiles[g])
        down = both
        pivots = jnp.ones((MB, BK), jnp.float32)
        scale = pivots
        p = over_rows(cols[0], 0)
        for k in range(MB):
            r = inverse_of(p)
            pivots = jnp.where(sub == k, p, pivots)
            scale = jnp.where(sub == k, r, scale)
            if k + 1 < MB and 1:
                b = over_rows(cols[k], k + 1)
                p = over_rows(cols[k + 1], k + 1) - (b * b) * r
            m = jnp.where(sub == k, 0.0, cols[k] * r)
            row = over_rows(both, k)
            for k2 in range(k + 1, MB):
                cols[k2] = cols[k2] - m * over_rows(cols[k2], k)
            if k + 1 < MB and not 1:
                p = over_rows(cols[k + 1], k + 1)
            both = both - m * row
            down = down - jnp.where(sub > k, m, 0.0) * row
        w_ref[pl.ds(pl.multiple_of(first + c0, MB), MB), :] = (
            jnp.where(lane < c0 + MB, down, 0.0) * lax.rsqrt(pivots))
        both = both * scale
        rows = [over_rows(both, k) for k in range(MB)]
        for i in range(g + 1, n):
            tile = jnp.where(own, 0.0, tiles[i])
            for k in range(MB):
                tile = tile - over_lanes(tiles[i], c0 + k) * rows[k]
            tiles[i] = tile


def factor_kernel(core_ref, mine_ref, other_ref, a_ref, w_ref):
    nb = TOP // BK
    pieces = mine_ref.shape[0]
    half = mine_ref.shape[1]
    per = pieces // (nb // 2)

    def place(first, second):
        for b in range(nb // 2):
            for i in range(per):
                for h, ref in enumerate((first, second)):
                    src = ref[b * per + i]
                    at = i * 2 * half + h * half
                    r = nb - 1 - b
                    a_ref[r * BK + at:r * BK + at + half, :(r + 1) * BK] = src[:, :(r + 1) * BK]
                    for j in range(b + 1):
                        a_ref[b * BK + at:b * BK + at + half, j * BK:(j + 1) * BK] = (
                            src[:, (nb - j) * BK:(nb + 1 - j) * BK])

    @pl.when(core_ref[0] == 0)
    def _():
        place(mine_ref, other_ref)

    @pl.when(core_ref[0] != 0)
    def _():
        place(other_ref, mine_ref)

    def step(j, carry):
        o = pl.multiple_of(j * BK, BK)
        tiles = [a_ref[pl.ds(pl.multiple_of(o + MB * i, MB), MB), pl.ds(o, BK)] for i in range(BK // MB)]
        invert_factor(tiles, w_ref, o)
        for b in range(nb - 1):
            @pl.when(j == b)
            def _():
                lo, hi = b * BK, (b + 1) * BK
                panel = long_dot(left(a_ref[hi:, lo:hi]), right(w_ref[lo:hi, :]))
                a_ref[hi:, lo:hi] = panel
                pl_, pr_ = left(panel), right(panel)
                for at in range(hi, TOP, 256):
                    to = min(at + 256, TOP)
                    a_ref[at:, at:to] -= long_dot(pl_[at - hi:], pr_[at - hi:to - hi])
        return carry

    lax.fori_loop(0, nb, step, 0)


def solve_kernel(first_ref, d0_ref, d1_ref, d2_ref, d3_ref, u0_ref, u1_ref, u2_ref, a_ref, w_ref, o_ref):
    nb = TOP // BK
    dist = (d0_ref[...] + d1_ref[...]) + (d2_ref[...] + d3_ref[...])
    update = (u0_ref[...] + u1_ref[...]) + u2_ref[...]
    rows = dist.shape[0]
    pos = first_ref[0] + lax.broadcasted_iota(jnp.int32, (rows, TOP), 0)
    col = lax.broadcasted_iota(jnp.int32, (rows, TOP), 1)
    shift = jnp.where(pos == col, RIDGE, 0.0)
    m = jnp.exp(-dist / (2.0 * F)) + shift - update
    for b in range(nb):
        lo, hi = b * BK, (b + 1) * BK
        x = long_dot(left(m[:, :BK]), right(w_ref[lo:hi, :]))
        keep = (pos[:, lo:hi] >= PW) | (lo < PW)
        o_ref[:, lo:hi] = jnp.where(keep, x, 0.0)
        if b + 1 < nb:
            m = m[:, BK:] - long_dot(left(x), right(a_ref[hi:, lo:hi]))


def factor(core, mine, other):
    vmem = pl.BlockSpec(memory_space=pltpu.VMEM)
    return pl.pallas_call(
        factor_kernel,
        out_shape=(jax.ShapeDtypeStruct((TOP, TOP), jnp.float32), jax.ShapeDtypeStruct((TOP, BK), jnp.float32)),
        in_specs=[pl.BlockSpec(memory_space=pltpu.SMEM), vmem, vmem],
        out_specs=(vmem, vmem),
    )(core, mine, other)


def solve(first, parts, low, inverses):
    vmem = pl.BlockSpec(memory_space=pltpu.VMEM)
    return pl.pallas_call(
        solve_kernel,
        out_shape=jax.ShapeDtypeStruct((parts[0].shape[0], TOP), jnp.float32),
        in_specs=[pl.BlockSpec(memory_space=pltpu.SMEM)] + [vmem] * (len(parts) + 2),
        out_specs=vmem,
    )(first, *parts, low, inverses)


def shards(features, slab, pack_order, place_order, start):
    n_krow, n_col = lax.axis_size("krow"), lax.axis_size("col")
    rows_dev = features.shape[0]
    group = rows_dev // n_krow
    prior_dev = slab.shape[1]
    krow, col = lax.axis_index("krow"), lax.axis_index("col")

    kept = (col * prior_dev + jnp.arange(prior_dev) < start[0])[None, :]
    order = place_order[0]
    coded = jnp.stack([order // CODE, order % CODE], axis=1).astype(jnp.bfloat16)
    coded = jnp.pad(coded, ((0, 0), (0, BK - 2)))
    packed = rows_at(features, pack_order[0])
    feat_dev = packed.shape[1]
    arrived = swap(jnp.concatenate([packed, slab, coded], axis=1), "krow")
    mine = jnp.concatenate([packed[:2 * group], arrived[:2 * group, feat_dev:]], axis=1)
    arrived = arrived[:, :feat_dev]
    tiles = from_everyone(mine, "krow")

    tiles = tiles.reshape(n_krow, 2, group, tiles.shape[-1])
    top = jnp.moveaxis(tiles, 1, 0).reshape(TOP, tiles.shape[-1])
    places = top[:, feat_dev + prior_dev:feat_dev + prior_dev + 2].astype(jnp.float32).astype(jnp.int32)
    wanted = (places[:, :1] * CODE + places[:, 1:]).reshape(2, rows_dev, 1)
    pick = (wanted == jnp.arange(rows_dev)).astype(jnp.bfloat16)
    top_feats = jnp.einsum("bij,bjf->bif", pick, top[:, :feat_dev].reshape(2, rows_dev, feat_dev),
                           preferred_element_type=jnp.float32).astype(jnp.bfloat16).reshape(TOP, feat_dev)
    top_slab = jnp.where(kept, top[:, feat_dev:feat_dev + prior_dev], jnp.zeros((), jnp.bfloat16))
    top_norms = sq_norms(top_feats)

    share = PW // n_krow
    at = krow * share
    pair = at // BK
    row_lo = at
    row_hi = (7 - pair) * BK + (at - pair * BK)

    def rows_of(array, first):
        return lax.dynamic_slice_in_dim(array, first, share, 0)

    def both(array):
        return jnp.concatenate([rows_of(array, row_hi), rows_of(array, row_lo)], axis=0)

    gram = inner(both(top_feats), top_feats)
    dist = both(top_norms)[:, None] + top_norms[None, :] - 2.0 * gram
    update = inner(both(top_slab), top_slab)
    dist = fold(dist[:share], dist[share:], pair)
    update = fold(update[:share], update[share:], pair)
    parts = jnp.concatenate([dist, update], axis=1)
    parts = swap(parts, "col")
    summed = jnp.sum(parts.reshape(n_col, share // n_col, 2 * 9 * BK), axis=0)
    dist, update = summed[:, :9 * BK], summed[:, 9 * BK:]
    mine = share // n_col
    ids = jnp.arange(mine)[:, None] + col * mine
    at_col = jnp.arange(9 * BK)[None, :]
    from_hi = at_col // BK + pair <= 7
    col_ids = jnp.where(from_hi, at_col, (8 - at_col // BK) * BK + at_col % BK)
    shift = (jnp.where(from_hi, row_hi, row_lo) + ids == col_ids).astype(jnp.float32)
    entries = jnp.exp(-dist / (2.0 * F)) + RIDGE * shift - update
    entries = from_everyone(entries, "col")
    entries = entries.reshape(share, 9 * BK)

    core, pair_at = col % 2, col // 2
    pairs = n_col // 2
    own = rows_dev // n_col

    def split_rows(array):
        array = array.reshape(pairs, 2, own, *array.shape[1:])
        halves = [lax.dynamic_index_in_dim(array, which, 1, keepdims=False) for which in (1 - core, core)]
        return jnp.concatenate([h.reshape(pairs * own, *h.shape[2:]) for h in halves], axis=0)

    def other_core(value):
        return lax.ppermute(value, "col", [(c, c ^ 1) for c in range(n_col)])

    def spread_over_pairs(value):
        pieces = [lax.dynamic_index_in_dim(value, pair_at, 0, keepdims=False)]
        for away in range(1, pairs):
            piece = lax.dynamic_index_in_dim(value, (pair_at + away) % pairs, 0, keepdims=False)
            to = [(c, (c // 2 + away) % pairs * 2 + c % 2) for c in range(n_col)]
            pieces.append(lax.ppermute(piece, "col", to))
        return pieces

    def relayed_over_pairs(value):
        def step(piece, by):
            return lax.ppermute(piece, "col", [(c, (c // 2 + by) % pairs * 2 + c % 2) for c in range(n_col)])

        def piece_at(away):
            return lax.dynamic_index_in_dim(value, (pair_at + away) % pairs, 0, keepdims=False)

        middle = own // 2
        opposite, nxt, prev = piece_at(2), piece_at(1), piece_at(pairs - 1)
        up = step(opposite[:middle], 1)
        down = step(opposite[middle:], -1)
        nxt = jnp.concatenate([nxt[:middle] + up, nxt[middle:]], axis=0)
        prev = jnp.concatenate([prev[:middle], prev[middle:] + down], axis=0)
        return [piece_at(0), step(nxt, 1), step(prev, -1)]

    half = pairs * own
    update = inner(split_rows(slab), top_slab)
    update_got = other_core(update[:half])
    updates = (update[half:] + update_got).reshape(pairs, own, TOP)
    updates = relayed_over_pairs(updates)

    ordered = rows_at(arrived, split_rows(place_order[0]))
    dist = sq_norms(ordered)[:, None] + top_norms[None, :] - 2.0 * inner(ordered, top_feats)
    dist_got = other_core(dist[:half])
    dists = (dist[half:] + dist_got).reshape(pairs, own, TOP)
    dists = spread_over_pairs(dists)

    half_share = share // 2
    piece = lax.dynamic_slice_in_dim(entries, core * half_share, half_share, 0)
    mine = from_everyone(piece, "krow")
    mine = mine.reshape(n_krow, half_share, 9 * BK)
    other = lax.ppermute(mine, "col", [(c, c ^ 1) for c in range(n_col)])
    low, inverses = factor(core.reshape(1), mine, other)
    first_row = krow * rows_dev + col * own
    return solve(first_row.reshape(1), dists + updates, low, inverses)


def solution(mesh):
    in_specs = (P("krow", "col"), P("krow", "col"), P("krow", None), P("krow", None), P())
    out_specs = P(("krow", "col"), None)
    return jax.shard_map(shards, mesh=mesh, in_specs=in_specs, out_specs=out_specs, check_vma=False)
```

```python
import jax
import jax.numpy as jnp
from jax import lax
from jax.experimental import pallas as pl
from jax.experimental.pallas import tpu as pltpu
from jax.sharding import PartitionSpec as P

F = 6144
PW = 512
TOP = 2 * PW
BK = 128
CODE = 32
MB = 16
RIDGE = 0.5


def rows_at(array, where):
    dims = lax.GatherDimensionNumbers(offset_dims=(1,), collapsed_slice_dims=(0,), start_index_map=(0,))
    return lax.gather(array, where[:, None], dims, (1, array.shape[1]), unique_indices=True,
                      mode=lax.GatherScatterMode.PROMISE_IN_BOUNDS)


def swap(value, axis):
    return lax.all_to_all(value, axis, split_axis=0, concat_axis=0, tiled=True)


def from_everyone(value, axis):
    return swap(jnp.broadcast_to(value, (lax.axis_size(axis), *value.shape)), axis)


def sq_norms(rows):
    return jnp.sum(jnp.square(rows.astype(jnp.float32)), axis=1)


def inner(a, b):
    return lax.dot_general(a, b, (((1,), (1,)), ((), ())), preferred_element_type=jnp.float32)


def fold(upper, lower, pair):
    blocks = []
    for slot in range(9):
        hi = upper[:, slot * BK:(slot + 1) * BK] if slot < 8 else None
        at = 8 - slot
        lo = lower[:, at * BK:(at + 1) * BK] if slot > 4 else None
        if lo is None:
            blocks.append(hi)
        elif hi is None:
            blocks.append(lo)
        else:
            blocks.append(jnp.where(slot + pair <= 7, hi, lo))
    return jnp.concatenate(blocks, axis=1)


def parts_of(x):
    high = x.astype(jnp.bfloat16)
    rest = x - high.astype(jnp.float32)
    mid = rest.astype(jnp.bfloat16)
    low = (rest - mid.astype(jnp.float32)).astype(jnp.bfloat16)
    return high, mid, low


def left(x):
    h, m, l = parts_of(x)
    return jnp.concatenate([h, h, m, m, h, l], axis=1)


def right(x):
    h, m, l = parts_of(x)
    return jnp.concatenate([h, m, h, m, l, h], axis=1)


def long_dot(a, b):
    return lax.dot_general(a, b, (((1,), (1,)), ((), ())), preferred_element_type=jnp.float32)


def over_rows(v, k):
    return jnp.broadcast_to(v[k:k + 1, :], v.shape)


def over_lanes(v, c):
    return jnp.take_along_axis(v, jnp.full(v.shape, c, jnp.int32), axis=1, mode="promise_in_bounds")


def inverse_of(p):
    return 1.0 / p


def invert_factor(tiles, w_ref, first):
    n = len(tiles)
    lane = lax.broadcasted_iota(jnp.int32, (MB, BK), 1)
    sub = lax.broadcasted_iota(jnp.int32, (MB, BK), 0)
    for g in range(n):
        c0 = MB * g
        cols = [over_lanes(tiles[g], c0 + k) for k in range(MB)]
        own = (lane >= c0) & (lane < c0 + MB)
        both = jnp.where(own, jnp.where(lane == c0 + sub, 1.0, 0.0), tiles[g])
        down = both
        pivots = jnp.ones((MB, BK), jnp.float32)
        scale = pivots
        p = over_rows(cols[0], 0)
        for k in range(MB):
            r = inverse_of(p)
            pivots = jnp.where(sub == k, p, pivots)
            scale = jnp.where(sub == k, r, scale)
            if k + 1 < MB and 1:
                b = over_rows(cols[k], k + 1)
                p = over_rows(cols[k + 1], k + 1) - (b * b) * r
            m = jnp.where(sub == k, 0.0, cols[k] * r)
            row = over_rows(both, k)
            for k2 in range(k + 1, MB):
                cols[k2] = cols[k2] - m * over_rows(cols[k2], k)
            if k + 1 < MB and not 1:
                p = over_rows(cols[k + 1], k + 1)
            both = both - m * row
            down = down - jnp.where(sub > k, m, 0.0) * row
        w_ref[pl.ds(pl.multiple_of(first + c0, MB), MB), :] = (
            jnp.where(lane < c0 + MB, down, 0.0) * lax.rsqrt(pivots))
        both = both * scale
        rows = [over_rows(both, k) for k in range(MB)]
        for i in range(g + 1, n):
            tile = jnp.where(own, 0.0, tiles[i])
            for k in range(MB):
                tile = tile - over_lanes(tiles[i], c0 + k) * rows[k]
            tiles[i] = tile


def factor_kernel(core_ref, mine_ref, other_ref, a_ref, w_ref):
    nb = TOP // BK
    pieces = mine_ref.shape[0]
    half = mine_ref.shape[1]
    per = pieces // (nb // 2)

    def place(first, second):
        for b in range(nb // 2):
            for i in range(per):
                for h, ref in enumerate((first, second)):
                    src = ref[b * per + i]
                    at = i * 2 * half + h * half
                    r = nb - 1 - b
                    a_ref[r * BK + at:r * BK + at + half, :(r + 1) * BK] = src[:, :(r + 1) * BK]
                    for j in range(b + 1):
                        a_ref[b * BK + at:b * BK + at + half, j * BK:(j + 1) * BK] = (
                            src[:, (nb - j) * BK:(nb + 1 - j) * BK])

    @pl.when(core_ref[0] == 0)
    def _():
        place(mine_ref, other_ref)

    @pl.when(core_ref[0] != 0)
    def _():
        place(other_ref, mine_ref)

    def step(j, carry):
        o = pl.multiple_of(j * BK, BK)
        tiles = [a_ref[pl.ds(pl.multiple_of(o + MB * i, MB), MB), pl.ds(o, BK)] for i in range(BK // MB)]
        invert_factor(tiles, w_ref, o)
        for b in range(nb - 1):
            @pl.when(j == b)
            def _():
                lo, hi = b * BK, (b + 1) * BK
                panel = long_dot(left(a_ref[hi:, lo:hi]), right(w_ref[lo:hi, :]))
                a_ref[hi:, lo:hi] = panel
                pl_, pr_ = left(panel), right(panel)
                for at in range(hi, TOP, 256):
                    to = min(at + 256, TOP)
                    a_ref[at:, at:to] -= long_dot(pl_[at - hi:], pr_[at - hi:to - hi])
        return carry

    lax.fori_loop(0, nb, step, 0)


def solve_kernel(first_ref, d0_ref, d1_ref, d2_ref, d3_ref, u0_ref, u1_ref, u2_ref, a_ref, w_ref, o_ref):
    nb = TOP // BK
    dist = (d0_ref[...] + d1_ref[...]) + (d2_ref[...] + d3_ref[...])
    update = (u0_ref[...] + u1_ref[...]) + u2_ref[...]
    rows = dist.shape[0]
    pos = first_ref[0] + lax.broadcasted_iota(jnp.int32, (rows, TOP), 0)
    col = lax.broadcasted_iota(jnp.int32, (rows, TOP), 1)
    shift = jnp.where(pos == col, RIDGE, 0.0)
    m = jnp.exp(-dist / (2.0 * F)) + shift - update
    for b in range(nb):
        lo, hi = b * BK, (b + 1) * BK
        x = long_dot(left(m[:, :BK]), right(w_ref[lo:hi, :]))
        keep = (pos[:, lo:hi] >= PW) | (lo < PW)
        o_ref[:, lo:hi] = jnp.where(keep, x, 0.0)
        if b + 1 < nb:
            m = m[:, BK:] - long_dot(left(x), right(a_ref[hi:, lo:hi]))


def factor(core, mine, other):
    vmem = pl.BlockSpec(memory_space=pltpu.VMEM)
    return pl.pallas_call(
        factor_kernel,
        out_shape=(jax.ShapeDtypeStruct((TOP, TOP), jnp.float32), jax.ShapeDtypeStruct((TOP, BK), jnp.float32)),
        in_specs=[pl.BlockSpec(memory_space=pltpu.SMEM), vmem, vmem],
        out_specs=(vmem, vmem),
    )(core, mine, other)


def solve(first, parts, low, inverses):
    vmem = pl.BlockSpec(memory_space=pltpu.VMEM)
    return pl.pallas_call(
        solve_kernel,
        out_shape=jax.ShapeDtypeStruct((parts[0].shape[0], TOP), jnp.float32),
        in_specs=[pl.BlockSpec(memory_space=pltpu.SMEM)] + [vmem] * (len(parts) + 2),
        out_specs=vmem,
    )(first, *parts, low, inverses)


def shards(features, slab, pack_order, place_order, start):
    n_krow, n_col = lax.axis_size("krow"), lax.axis_size("col")
    rows_dev = features.shape[0]
    group = rows_dev // n_krow
    prior_dev = slab.shape[1]
    krow, col = lax.axis_index("krow"), lax.axis_index("col")

    kept = (col * prior_dev + jnp.arange(prior_dev) < start[0])[None, :]
    order = place_order[0]
    coded = jnp.stack([order // CODE, order % CODE], axis=1).astype(jnp.bfloat16)
    coded = jnp.pad(coded, ((0, 0), (0, BK - 2)))
    packed = rows_at(features, pack_order[0])
    feat_dev = packed.shape[1]
    arrived = swap(jnp.concatenate([packed, slab, coded], axis=1), "krow")
    core, pair_at = col % 2, col // 2
    pairs = n_col // 2
    own = rows_dev // n_col

    def split_rows(array):
        array = array.reshape(pairs, 2, own, *array.shape[1:])
        halves = [lax.dynamic_index_in_dim(array, which, 1, keepdims=False) for which in (1 - core, core)]
        return jnp.concatenate([h.reshape(pairs * own, *h.shape[2:]) for h in halves], axis=0)

    mine = jnp.concatenate([packed[:2 * group], arrived[:2 * group, feat_dev:]], axis=1)
    tiles = from_everyone(mine, "krow")
    own_places = split_rows(place_order[0])
    ordered = rows_at(arrived[:, :feat_dev], own_places)
    own_norms = sq_norms(ordered)

    tiles = tiles.reshape(n_krow, 2, group, tiles.shape[-1])
    top = jnp.moveaxis(tiles, 1, 0).reshape(TOP, tiles.shape[-1])
    places = top[:, feat_dev + prior_dev:feat_dev + prior_dev + 2].astype(jnp.float32).astype(jnp.int32)
    wanted = (places[:, :1] * CODE + places[:, 1:]).reshape(2, rows_dev, 1)
    pick = (wanted == jnp.arange(rows_dev)).astype(jnp.bfloat16)
    top_feats = jnp.einsum("bij,bjf->bif", pick, top[:, :feat_dev].reshape(2, rows_dev, feat_dev),
                           preferred_element_type=jnp.float32).astype(jnp.bfloat16).reshape(TOP, feat_dev)
    top_slab = jnp.where(kept, top[:, feat_dev:feat_dev + prior_dev], jnp.zeros((), jnp.bfloat16))
    top_norms = sq_norms(top_feats)

    share = PW // n_krow
    at = krow * share
    pair = at // BK
    row_lo = at
    row_hi = (7 - pair) * BK + (at - pair * BK)

    def rows_of(array, first):
        return lax.dynamic_slice_in_dim(array, first, share, 0)

    def both(array):
        return jnp.concatenate([rows_of(array, row_hi), rows_of(array, row_lo)], axis=0)

    gram = inner(both(top_feats), top_feats)
    dist = both(top_norms)[:, None] + top_norms[None, :] - 2.0 * gram
    update = inner(both(top_slab), top_slab)
    dist = fold(dist[:share], dist[share:], pair)
    update = fold(update[:share], update[share:], pair)
    parts = jnp.concatenate([dist, update], axis=1)
    parts = swap(parts, "col")
    summed = jnp.sum(parts.reshape(n_col, share // n_col, 2 * 9 * BK), axis=0)
    dist, update = summed[:, :9 * BK], summed[:, 9 * BK:]
    mine = share // n_col
    ids = jnp.arange(mine)[:, None] + col * mine
    at_col = jnp.arange(9 * BK)[None, :]
    from_hi = at_col // BK + pair <= 7
    col_ids = jnp.where(from_hi, at_col, (8 - at_col // BK) * BK + at_col % BK)
    shift = (jnp.where(from_hi, row_hi, row_lo) + ids == col_ids).astype(jnp.float32)
    entries = jnp.exp(-dist / (2.0 * F)) + RIDGE * shift - update
    entries = from_everyone(entries, "col")
    entries = entries.reshape(share, 9 * BK)

    def other_core(value):
        return lax.ppermute(value, "col", [(c, c ^ 1) for c in range(n_col)])

    def spread_over_pairs(value):
        pieces = [lax.dynamic_index_in_dim(value, pair_at, 0, keepdims=False)]
        for away in range(1, pairs):
            piece = lax.dynamic_index_in_dim(value, (pair_at + away) % pairs, 0, keepdims=False)
            to = [(c, (c // 2 + away) % pairs * 2 + c % 2) for c in range(n_col)]
            pieces.append(lax.ppermute(piece, "col", to))
        return pieces

    def relayed_over_pairs(value):
        def step(piece, by):
            return lax.ppermute(piece, "col", [(c, (c // 2 + by) % pairs * 2 + c % 2) for c in range(n_col)])

        def piece_at(away):
            return lax.dynamic_index_in_dim(value, (pair_at + away) % pairs, 0, keepdims=False)

        middle = own // 2
        opposite, nxt, prev = piece_at(2), piece_at(1), piece_at(pairs - 1)
        up = step(opposite[:middle], 1)
        down = step(opposite[middle:], -1)
        nxt = jnp.concatenate([nxt[:middle] + up, nxt[middle:]], axis=0)
        prev = jnp.concatenate([prev[:middle], prev[middle:] + down], axis=0)
        kept_piece = piece_at(0)
        return [kept_piece, step(nxt, 1), step(prev, -1)]

    half = pairs * own
    update = inner(split_rows(slab), top_slab)
    update_got = other_core(update[:half])
    updates = (update[half:] + update_got).reshape(pairs, own, TOP)
    updates = relayed_over_pairs(updates)

    dist = own_norms[:, None] + top_norms[None, :] - 2.0 * inner(ordered, top_feats)
    dist_got = other_core(dist[:half])
    dists = (dist[half:] + dist_got).reshape(pairs, own, TOP)
    dists = spread_over_pairs(dists)

    half_share = share // 2
    piece = lax.dynamic_slice_in_dim(entries, core * half_share, half_share, 0)
    mine = from_everyone(piece, "krow")
    mine = mine.reshape(n_krow, half_share, 9 * BK)
    other = lax.ppermute(mine, "col", [(c, c ^ 1) for c in range(n_col)])
    low, inverses = factor(core.reshape(1), mine, other)
    first_row = krow * rows_dev + col * own
    return solve(first_row.reshape(1), dists + updates, low, inverses)


def solution(mesh):
    in_specs = (P("krow", "col"), P("krow", "col"), P("krow", None), P("krow", None), P())
    out_specs = P(("krow", "col"), None)
    return jax.shard_map(shards, mesh=mesh, in_specs=in_specs, out_specs=out_specs, check_vma=False)
```

```python
import jax
import jax.numpy as jnp
from jax import lax
from jax.experimental import pallas as pl
from jax.experimental.pallas import tpu as pltpu
from jax.sharding import PartitionSpec as P

F = 6144
PW = 512
TOP = 2 * PW
BK = 128
CODE = 32
MB = 16
RIDGE = 0.5


def rows_at(array, where):
    dims = lax.GatherDimensionNumbers(offset_dims=(1,), collapsed_slice_dims=(0,), start_index_map=(0,))
    return lax.gather(array, where[:, None], dims, (1, array.shape[1]), unique_indices=True,
                      mode=lax.GatherScatterMode.PROMISE_IN_BOUNDS)


def swap(value, axis):
    return lax.all_to_all(value, axis, split_axis=0, concat_axis=0, tiled=True)


def from_everyone(value, axis):
    return swap(jnp.broadcast_to(value, (lax.axis_size(axis), *value.shape)), axis)


def sq_norms(rows):
    return jnp.sum(jnp.square(rows.astype(jnp.float32)), axis=1)


def inner(a, b):
    return lax.dot_general(a, b, (((1,), (1,)), ((), ())), preferred_element_type=jnp.float32)


def fold(upper, lower, pair):
    blocks = []
    for slot in range(9):
        hi = upper[:, slot * BK:(slot + 1) * BK] if slot < 8 else None
        at = 8 - slot
        lo = lower[:, at * BK:(at + 1) * BK] if slot > 4 else None
        if lo is None:
            blocks.append(hi)
        elif hi is None:
            blocks.append(lo)
        else:
            blocks.append(jnp.where(slot + pair <= 7, hi, lo))
    return jnp.concatenate(blocks, axis=1)


def parts_of(x):
    high = x.astype(jnp.bfloat16)
    rest = x - high.astype(jnp.float32)
    mid = rest.astype(jnp.bfloat16)
    low = (rest - mid.astype(jnp.float32)).astype(jnp.bfloat16)
    return high, mid, low


def left(x):
    h, m, l = parts_of(x)
    return jnp.concatenate([h, h, m, m, h, l], axis=1)


def right(x):
    h, m, l = parts_of(x)
    return jnp.concatenate([h, m, h, m, l, h], axis=1)


def long_dot(a, b):
    return lax.dot_general(a, b, (((1,), (1,)), ((), ())), preferred_element_type=jnp.float32)


def over_rows(v, k):
    return jnp.broadcast_to(v[k:k + 1, :], v.shape)


def over_lanes(v, c):
    return jnp.take_along_axis(v, jnp.full(v.shape, c, jnp.int32), axis=1, mode="promise_in_bounds")


def inverse_of(p):
    return 1.0 / p


def invert_factor(tiles, w_ref, first):
    n = len(tiles)
    lane = lax.broadcasted_iota(jnp.int32, (MB, BK), 1)
    sub = lax.broadcasted_iota(jnp.int32, (MB, BK), 0)
    for g in range(n):
        c0 = MB * g
        cols = [over_lanes(tiles[g], c0 + k) for k in range(MB)]
        own = (lane >= c0) & (lane < c0 + MB)
        both = jnp.where(own, jnp.where(lane == c0 + sub, 1.0, 0.0), tiles[g])
        down = both
        pivots = jnp.ones((MB, BK), jnp.float32)
        scale = pivots
        p = over_rows(cols[0], 0)
        for k in range(MB):
            r = inverse_of(p)
            pivots = jnp.where(sub == k, p, pivots)
            scale = jnp.where(sub == k, r, scale)
            if k + 1 < MB and 1:
                b = over_rows(cols[k], k + 1)
                p = over_rows(cols[k + 1], k + 1) - (b * b) * r
            m = jnp.where(sub == k, 0.0, cols[k] * r)
            row = over_rows(both, k)
            for k2 in range(k + 1, MB):
                cols[k2] = cols[k2] - m * over_rows(cols[k2], k)
            if k + 1 < MB and not 1:
                p = over_rows(cols[k + 1], k + 1)
            both = both - m * row
            down = down - jnp.where(sub > k, m, 0.0) * row
        w_ref[pl.ds(pl.multiple_of(first + c0, MB), MB), :] = (
            jnp.where(lane < c0 + MB, down, 0.0) * lax.rsqrt(pivots))
        both = both * scale
        rows = [over_rows(both, k) for k in range(MB)]
        for i in range(g + 1, n):
            tile = jnp.where(own, 0.0, tiles[i])
            for k in range(MB):
                tile = tile - over_lanes(tiles[i], c0 + k) * rows[k]
            tiles[i] = tile


def factor_kernel(core_ref, mine_ref, other_ref, a_ref, w_ref):
    nb = TOP // BK
    pieces = mine_ref.shape[0]
    half = mine_ref.shape[1]
    per = pieces // (nb // 2)

    def place(first, second):
        for b in range(nb // 2):
            for i in range(per):
                for h, ref in enumerate((first, second)):
                    src = ref[b * per + i]
                    at = i * 2 * half + h * half
                    r = nb - 1 - b
                    a_ref[r * BK + at:r * BK + at + half, :(r + 1) * BK] = src[:, :(r + 1) * BK]
                    for j in range(b + 1):
                        a_ref[b * BK + at:b * BK + at + half, j * BK:(j + 1) * BK] = (
                            src[:, (nb - j) * BK:(nb + 1 - j) * BK])

    @pl.when(core_ref[0] == 0)
    def _():
        place(mine_ref, other_ref)

    @pl.when(core_ref[0] != 0)
    def _():
        place(other_ref, mine_ref)

    def step(j, carry):
        o = pl.multiple_of(j * BK, BK)
        tiles = [a_ref[pl.ds(pl.multiple_of(o + MB * i, MB), MB), pl.ds(o, BK)] for i in range(BK // MB)]
        invert_factor(tiles, w_ref, o)
        for b in range(nb - 1):
            @pl.when(j == b)
            def _():
                lo, hi = b * BK, (b + 1) * BK
                panel = long_dot(left(a_ref[hi:, lo:hi]), right(w_ref[lo:hi, :]))
                a_ref[hi:, lo:hi] = panel
                pl_, pr_ = left(panel), right(panel)
                for at in range(hi, TOP, 256):
                    to = min(at + 256, TOP)
                    a_ref[at:, at:to] -= long_dot(pl_[at - hi:], pr_[at - hi:to - hi])
        return carry

    lax.fori_loop(0, nb, step, 0)


def solve_kernel(first_ref, d0_ref, d1_ref, d2_ref, d3_ref, u0_ref, u1_ref, u2_ref, a_ref, w_ref, o_ref):
    nb = TOP // BK
    dist = (d0_ref[...] + d1_ref[...]) + (d2_ref[...] + d3_ref[...])
    update = (u0_ref[...] + u1_ref[...]) + u2_ref[...]
    rows = dist.shape[0]
    pos = first_ref[0] + lax.broadcasted_iota(jnp.int32, (rows, TOP), 0)
    col = lax.broadcasted_iota(jnp.int32, (rows, TOP), 1)
    shift = jnp.where(pos == col, RIDGE, 0.0)
    m = jnp.exp(-dist / (2.0 * F)) + shift - update
    for b in range(nb):
        lo, hi = b * BK, (b + 1) * BK
        x = long_dot(left(m[:, :BK]), right(w_ref[lo:hi, :]))
        keep = (pos[:, lo:hi] >= PW) | (lo < PW)
        o_ref[:, lo:hi] = jnp.where(keep, x, 0.0)
        if b + 1 < nb:
            m = m[:, BK:] - long_dot(left(x), right(a_ref[hi:, lo:hi]))


def factor(core, mine, other):
    vmem = pl.BlockSpec(memory_space=pltpu.VMEM)
    return pl.pallas_call(
        factor_kernel,
        out_shape=(jax.ShapeDtypeStruct((TOP, TOP), jnp.float32), jax.ShapeDtypeStruct((TOP, BK), jnp.float32)),
        in_specs=[pl.BlockSpec(memory_space=pltpu.SMEM), vmem, vmem],
        out_specs=(vmem, vmem),
    )(core, mine, other)


def solve(first, parts, low, inverses):
    vmem = pl.BlockSpec(memory_space=pltpu.VMEM)
    return pl.pallas_call(
        solve_kernel,
        out_shape=jax.ShapeDtypeStruct((parts[0].shape[0], TOP), jnp.float32),
        in_specs=[pl.BlockSpec(memory_space=pltpu.SMEM)] + [vmem] * (len(parts) + 2),
        out_specs=vmem,
    )(first, *parts, low, inverses)


def shards(features, slab, pack_order, place_order, start):
    n_krow, n_col = lax.axis_size("krow"), lax.axis_size("col")
    rows_dev = features.shape[0]
    group = rows_dev // n_krow
    prior_dev = slab.shape[1]
    krow, col = lax.axis_index("krow"), lax.axis_index("col")

    kept = (col * prior_dev + jnp.arange(prior_dev) < start[0])[None, :]
    order = place_order[0]
    coded = jnp.stack([order // CODE, order % CODE], axis=1).astype(jnp.bfloat16)
    coded = jnp.pad(coded, ((0, 0), (0, BK - 2)))
    packed = rows_at(features, pack_order[0])
    feat_dev = packed.shape[1]
    arrived = swap(jnp.concatenate([packed, slab, coded], axis=1), "krow")
    mine = jnp.concatenate([packed[:2 * group], arrived[:2 * group, feat_dev:]], axis=1)
    arrived = arrived[:, :feat_dev]
    tiles = from_everyone(mine, "krow")

    tiles = tiles.reshape(n_krow, 2, group, tiles.shape[-1])
    top = jnp.moveaxis(tiles, 1, 0).reshape(TOP, tiles.shape[-1])
    places = top[:, feat_dev + prior_dev:feat_dev + prior_dev + 2].astype(jnp.float32).astype(jnp.int32)
    wanted = (places[:, :1] * CODE + places[:, 1:]).reshape(2, rows_dev, 1)
    pick = (wanted == jnp.arange(rows_dev)).astype(jnp.bfloat16)
    top_feats = jnp.einsum("bij,bjf->bif", pick, top[:, :feat_dev].reshape(2, rows_dev, feat_dev),
                           preferred_element_type=jnp.float32).astype(jnp.bfloat16).reshape(TOP, feat_dev)
    top_slab = jnp.where(kept, top[:, feat_dev:feat_dev + prior_dev], jnp.zeros((), jnp.bfloat16))
    top_norms = sq_norms(top_feats)

    share = PW // n_krow
    at = krow * share
    pair = at // BK
    row_lo = at
    row_hi = (7 - pair) * BK + (at - pair * BK)

    def rows_of(array, first):
        return lax.dynamic_slice_in_dim(array, first, share, 0)

    def both(array):
        return jnp.concatenate([rows_of(array, row_hi), rows_of(array, row_lo)], axis=0)

    gram = inner(both(top_feats), top_feats)
    dist = both(top_norms)[:, None] + top_norms[None, :] - 2.0 * gram
    update = inner(both(top_slab), top_slab)
    dist = fold(dist[:share], dist[share:], pair)
    update = fold(update[:share], update[share:], pair)
    parts = jnp.concatenate([dist, update], axis=1)
    parts = swap(parts, "col")
    summed = jnp.sum(parts.reshape(n_col, share // n_col, 2 * 9 * BK), axis=0)
    dist, update = summed[:, :9 * BK], summed[:, 9 * BK:]
    mine = share // n_col
    ids = jnp.arange(mine)[:, None] + col * mine
    at_col = jnp.arange(9 * BK)[None, :]
    from_hi = at_col // BK + pair <= 7
    col_ids = jnp.where(from_hi, at_col, (8 - at_col // BK) * BK + at_col % BK)
    shift = (jnp.where(from_hi, row_hi, row_lo) + ids == col_ids).astype(jnp.float32)
    entries = jnp.exp(-dist / (2.0 * F)) + RIDGE * shift - update
    entries = from_everyone(entries, "col")
    entries = entries.reshape(share, 9 * BK)

    core, pair_at = col % 2, col // 2
    pairs = n_col // 2
    own = rows_dev // n_col

    def split_rows(array):
        array = array.reshape(pairs, 2, own, *array.shape[1:])
        halves = [lax.dynamic_index_in_dim(array, which, 1, keepdims=False) for which in (1 - core, core)]
        return jnp.concatenate([h.reshape(pairs * own, *h.shape[2:]) for h in halves], axis=0)

    def other_core(value):
        return lax.ppermute(value, "col", [(c, c ^ 1) for c in range(n_col)])

    def spread_over_pairs(value):
        pieces = [lax.dynamic_index_in_dim(value, pair_at, 0, keepdims=False)]
        for away in range(1, pairs):
            piece = lax.dynamic_index_in_dim(value, (pair_at + away) % pairs, 0, keepdims=False)
            to = [(c, (c // 2 + away) % pairs * 2 + c % 2) for c in range(n_col)]
            pieces.append(lax.ppermute(piece, "col", to))
        return pieces

    def relayed_over_pairs(value):
        def step(piece, by):
            return lax.ppermute(piece, "col", [(c, (c // 2 + by) % pairs * 2 + c % 2) for c in range(n_col)])

        def piece_at(away):
            return lax.dynamic_index_in_dim(value, (pair_at + away) % pairs, 0, keepdims=False)

        middle = own // 2
        opposite, nxt, prev = piece_at(2), piece_at(1), piece_at(pairs - 1)
        up = step(opposite[:middle], 1)
        down = step(opposite[middle:], -1)
        nxt = jnp.concatenate([nxt[:middle] + up, nxt[middle:]], axis=0)
        prev = jnp.concatenate([prev[:middle], prev[middle:] + down], axis=0)
        kept_piece = piece_at(0)
        return [kept_piece, step(nxt, 1), step(prev, -1)]

    half = pairs * own
    update = inner(split_rows(slab), top_slab)
    update_got = other_core(update[:half])
    updates = (update[half:] + update_got).reshape(pairs, own, TOP)
    updates = relayed_over_pairs(updates)

    own_places = split_rows(place_order[0])
    ordered = rows_at(arrived, own_places)
    dist = sq_norms(ordered)[:, None] + top_norms[None, :] - 2.0 * inner(ordered, top_feats)
    dist_got = other_core(dist[:half])
    dists = (dist[half:] + dist_got).reshape(pairs, own, TOP)
    dists = spread_over_pairs(dists)

    half_share = share // 2
    piece = lax.dynamic_slice_in_dim(entries, core * half_share, half_share, 0)
    mine = from_everyone(piece, "krow")
    mine = mine.reshape(n_krow, half_share, 9 * BK)
    other = lax.ppermute(mine, "col", [(c, c ^ 1) for c in range(n_col)])
    low, inverses = factor(core.reshape(1), mine, other)
    first_row = krow * rows_dev + col * own
    return solve(first_row.reshape(1), dists + updates, low, inverses)


def solution(mesh):
    in_specs = (P("krow", "col"), P("krow", "col"), P("krow", None), P("krow", None), P())
    out_specs = P(("krow", "col"), None)
    return jax.shard_map(shards, mesh=mesh, in_specs=in_specs, out_specs=out_specs, check_vma=False)
```
